32 devices in a mesh: date: 16 (over z, y, x), prod: 2 (over core).
Axes of the slice: x: 2, y: 2, z: 4, core: 2. Of those that a mesh axis runs over, the one named last changes fastest.
Arguments:
- daily_sales: float32 [256, 512, 128], P('prod', 'date'), may hold values from -2.5 to 2.5
- week_id: int32 [512], P('date'), may hold values from 0 to 102, never falling along the last dimension, each value on 1 to 7 neighbouring positions
- month_id: int32 [512], P('date'), may hold values from 0 to 21, never falling along the last dimension, each value on 1 to 31 neighbouring positions
- year_id: int32 [512], P('date'), may hold values from 0 to 1, never falling along the last dimension, each value on 1 to 366 neighbouring positions
Outputs:
- running: float32 [256, 512, 128], P('prod', 'date')
- week_total: float32 [256, 512, 128], P('prod', 'date')
- month_total: float32 [256, 512, 128], P('prod', 'date')
- year_total: float32 [256, 512, 128], P('prod', 'date')
- store_rollup: float32 [4, 512, 128], P(None, 'date')
The draws below stay inside these ranges and needn't reach their ends.
Inputs may be any that keep to these rules, and one draw needn't show every extreme that they name: `week_id`: starts at 0 and never falls along the dates; each week covers 1 to 7 consecutive dates and some cover exactly 7. `month_id`: starts at 0 and never falls along the dates; each month covers 1 to 31 consecutive dates and some cover exactly 31; months need not line up with weeks. `year_id`: starts at 0 and never falls along the dates; each year covers 1 to 366 consecutive dates and some cover exactly 366; years need not line up with weeks or months.
All inputs are finite; a program needn't handle non-finite values.
Results may differ from the reference program's by a relative error of at most 0.000094.
Values sent between devices are 32-bit elements.
A program may use at most 64 MiB of HBM per device.

```python
import math
import jax
import jax.numpy as jnp
import numpy as np

PRODUCTS = 256
STORES = 128
DATES = 512


def shard_levels(stream_key, extent, split, low, high):
    loudness = 1.0
    for position, shards_of in split:
        steps = jax.random.uniform(jax.random.fold_in(jax.random.fold_in(stream_key, 6), position), (shards_of,), jnp.float32, low / len(split), high / len(split))
        loudness = loudness * jnp.repeat(jnp.exp(steps), extent[position] // shards_of).reshape((-1,) + (1,) * (len(extent) - 1 - position))
    return loudness


def split_up(number_of, total, reach, lean):
    portions = [(1 << 20) // math.isqrt(rank ** lean) + 1 for rank in range(2, number_of + 1)]
    rest, holding = total - reach - (number_of - 1), [1] * (number_of - 1)
    while rest > 0:
        movable = [i for i in range(number_of - 1) if holding[i] < reach]
        mass, remaining = sum([portions[i] for i in movable]), rest
        for i in movable:
            extra = min(reach - holding[i], max(1, remaining * portions[i] // mass), rest)
            holding[i] = holding[i] + extra
            rest = rest - extra
    return np.array([reach] + holding)


def uneven_parts(stream_key, amount, total, limit, slope):
    if amount == 2:
        one = jax.random.randint(stream_key, (), max(1, total - limit), min(limit, total - 1) + 1)
        return jnp.stack([one, total - one])
    tallies = jnp.asarray(split_up(amount, total, limit, slope), jnp.int32)
    pairs = (amount - 1) // 2
    giver, sink = tallies[1:1 + 2 * pairs:2], tallies[2:2 + 2 * pairs:2]
    room = jnp.minimum(giver - 1, limit - sink)
    passed = jax.random.randint(jax.random.fold_in(stream_key, 1), (pairs,), 0, 1 << 20) % (room + 1)
    tallies = tallies.at[1:1 + 2 * pairs:2].set(giver - passed).at[2:2 + 2 * pairs:2].set(sink + passed)
    return tallies[jax.random.permutation(jax.random.fold_in(stream_key, 2), amount)]


def normal_values(own_key, shape, deviation, limit, pieces=(), kind=jnp.bfloat16):
    factor_of = shard_levels(own_key, shape, pieces, -0.22, 0.18) if pieces else 1.0
    result = jax.random.normal(own_key, shape, jnp.float32) * deviation * factor_of
    return jnp.minimum(jnp.maximum(result, -limit), limit).astype(kind)


def setup_inputs(seed: int = 0) -> dict:
    seeds = jax.random.split(jax.random.key(seed), 5)
    return {
        "daily_sales": normal_values(seeds[0], (PRODUCTS, DATES, STORES), 0.25, 2.5, ((0, 2), (1, 16)), jnp.float32),
        "week_id": jnp.searchsorted(jnp.cumsum(uneven_parts(seeds[1], DATES // 5 + 1, DATES, 7, 0)), jnp.arange(DATES), side="right").astype(jnp.int32),
        "month_id": jnp.searchsorted(jnp.cumsum(uneven_parts(seeds[2], DATES // 24 + 1, DATES, 31, 0)), jnp.arange(DATES), side="right").astype(jnp.int32),
        "year_id": jnp.searchsorted(jnp.cumsum(uneven_parts(seeds[3], DATES // 300 + 1, DATES, 366, 0)), jnp.arange(DATES), side="right").astype(jnp.int32),
    }


def segment_totals(daily_sales, level_ids):
    by_date = jnp.moveaxis(daily_sales, 1, 0)
    seg_sums = jax.ops.segment_sum(by_date, level_ids, num_segments=DATES)
    return jnp.moveaxis(seg_sums[level_ids], 0, 1)


def reference(daily_sales, week_id, month_id, year_id):
    running = jnp.cumsum(daily_sales, axis=1)
    week_total = segment_totals(daily_sales, week_id)
    month_total = segment_totals(daily_sales, month_id)
    year_total = segment_totals(daily_sales, year_id)
    store_rollup = jnp.stack([jnp.sum(running, axis=0), jnp.sum(week_total, axis=0), jnp.sum(month_total, axis=0), jnp.sum(year_total, axis=0)])
    return running, week_total, month_total, year_total, store_rollup
```

```python
import functools

import jax
import jax.numpy as jnp
from jax import lax
from jax.experimental import pallas as pl
from jax.experimental.pallas import tpu as pltpu
from jax.sharding import PartitionSpec as P

MESH = pl.DeviceIdType.MESH
F32 = jnp.float32


def id_column(ids, span, lanes):
    where = lax.broadcasted_iota(jnp.int32, (span, lanes), 0)
    column = jnp.zeros((span, lanes), jnp.int32)
    for t in range(span):
        column = jnp.where(where == t, ids[t], column)
    return column


def id_row(ids, span, lanes):
    where = lax.broadcasted_iota(jnp.int32, (span, lanes), 1) % span
    row = jnp.zeros((span, lanes), jnp.int32)
    for t in range(span):
        row = jnp.where(where == t, ids[t], row)
    return row


def edge_masks(ids, span, lanes):
    column = id_column(ids, span, lanes)
    return (column == ids[0]).astype(F32), (column == ids[span - 1]).astype(F32)


def stack_rows(values, rows, lanes):
    where = lax.broadcasted_iota(jnp.int32, (rows, lanes), 0)
    tile = jnp.zeros((rows, lanes), F32)
    for i, value in enumerate(values):
        tile = jnp.where(where == i, value, tile)
    return tile


def split2(value):
    high = value.astype(jnp.bfloat16)
    low = (value - high.astype(F32)).astype(jnp.bfloat16)
    return jnp.concatenate([high, low], axis=-2)


def exchange_kernel(
    n, n_prod, m, slices, loads, wide,
    week_hbm, month_hbm, year_hbm, x_hbm,
    run_out, week_out, month_out, year_out, carry, cross, gains, coef, rollup,
    week, month, year, mixer, x, send1, recv1, send2, half, edges, near, beside, info, far, parts,
    ids_sem, load_sem, ready, i_s, i_r, s1_s, s1_r, s2_s, s2_r, c_s, c_r, f_s, f_r, sib_s, sib_r, near_s, near_r, b_s, b_r,
):
    me = lax.axis_index("date")
    core = lax.axis_index("prod")
    columns, span, lanes = x.shape
    rows = columns // slices
    chunk = columns // loads
    last = span - 1
    upper = me >= m
    lower = me < m
    base = jnp.where(upper, m, 0)
    there = m - base
    here = me - base
    order = sorted(range(1, m), key=lambda d: -min(d, m - d))
    loaded = [
        pltpu.make_async_copy(
            x_hbm.at[pl.ds(i * chunk, chunk)], x.at[pl.ds(i * chunk, chunk)], load_sem.at[i]
        )
        for i in range(loads)
    ]
    fetched = [
        pltpu.make_async_copy(source, target, ids_sem.at[i])
        for i, (source, target) in enumerate(
            ((year_hbm, year), (week_hbm, week), (month_hbm, month))
        )
    ]
    for copy in fetched + loaded:
        copy.start()

    barrier = pltpu.get_barrier_semaphore()

    def greet(date, prod):
        pl.semaphore_signal(barrier, inc=1, device_id=(date, prod), device_id_type=MESH)

    @pl.when(lower)
    def _():
        for j in reversed(range(m)):
            greet(m + j, core)

    for d in order:
        greet(base + lax.rem(here + d, m), core)
    for d in range(1, n_prod):
        greet(me, lax.rem(core + d, n_prod))

    @pl.when(me == m)
    def _():
        greet(m - 1, core)

    for copy in fetched:
        copy.wait()
    head_y, tail_y = edge_masks(year, span, lanes)
    head_w, tail_w = edge_masks(week, span, lanes)
    head_m, tail_m = edge_masks(month, span, lanes)
    lane = lax.broadcasted_iota(jnp.int32, (1, lanes), 1)
    ids = jnp.zeros((1, lanes), F32)
    for i, v in enumerate((year[0], year[last], week[0], week[last], month[0], month[last])):
        ids = jnp.where(lane == i, v.astype(F32), ids)
    wider = 2 * span
    sub = lax.broadcasted_iota(jnp.int32, (span, wider), 0)
    place = lax.broadcasted_iota(jnp.int32, (span, wider), 1) % span
    mixer[0:span] = jnp.where(place <= sub, 1.0, 0.0).astype(mixer.dtype)
    for k, level in enumerate((year, week, month)):
        same = id_column(level, span, wider) == id_row(level, span, wider)
        mixer[(k + 1) * span : (k + 2) * span] = jnp.where(same, 1.0, 0.0).astype(mixer.dtype)

    @pl.when(lower)
    def _():
        for j in range(m):
            cross[j, 0] = jnp.zeros((rows, lanes), F32)

    @pl.when(me == 0)
    def _():
        near[0] = jnp.zeros(near.shape[1:], F32)
        beside[0] = jnp.zeros(beside.shape[1:], F32)

    @pl.when(me == n - 1)
    def _():
        near[1] = jnp.zeros(near.shape[1:], F32)
        beside[1] = jnp.zeros(beside.shape[1:], F32)

    def outer_sums(s, total):
        block = x[pl.ds(pl.multiple_of(s * rows, rows), rows)]
        send1[s, 0] = jnp.sum(block * head_y[None], axis=1)
        send1[s, 1] = jnp.sum(block, axis=1)
        if wide:
            send1[s, 2] = jnp.sum(block * tail_y[None], axis=1)
        return total + jnp.sum(block, axis=0)

    total = jnp.zeros((span, lanes), F32)
    per_load = slices // loads
    for i in range(loads):
        loaded[i].wait()
        total = lax.fori_loop(i * per_load, (i + 1) * per_load, outer_sums, total)
    info[here] = stack_rows(
        [jnp.sum(total, axis=0, keepdims=True)]
        + [
            jnp.sum(total * mask, axis=0, keepdims=True)
            for mask in (head_y, tail_y, head_w, tail_w, head_m, tail_m)
        ]
        + [ids],
        8, lanes,
    )
    recv1[here] = send1[lax.rem(here, slices)]
    pl.semaphore_wait(
        barrier,
        m - 1 + n_prod - 1 + jnp.where(upper, m, 0) + jnp.where(me == m - 1, 1, 0),
    )

    @pl.when(upper)
    def _():
        for j in range(m):
            pl.semaphore_signal(ready, inc=1, device_id=(j, core), device_id_type=MESH)

    def to_mates(source, target, send_sem, recv_sem):
        copies = []
        for d in order:
            peer = lax.rem(here + d, m)
            copy = pltpu.make_async_remote_copy(
                src_ref=source(peer), dst_ref=target.at[here],
                send_sem=send_sem.at[peer], recv_sem=recv_sem.at[here],
                device_id=(base + peer, core), device_id_type=MESH,
            )
            copy.start()
            copies.append(copy)
        return copies

    def from_mates(target, send_sem, recv_sem):
        for d in order:
            peer = lax.rem(here + d, m)
            pltpu.make_async_remote_copy(
                src_ref=target.at[here], dst_ref=target.at[peer],
                send_sem=send_sem.at[peer], recv_sem=recv_sem.at[peer],
                device_id=(base + peer, core), device_id_type=MESH,
            ).wait_recv()

    sent = to_mates(lambda peer: info.at[here], info, i_s, i_r)
    sent += to_mates(lambda peer: send1.at[lax.rem(peer, slices)], recv1, s1_s, s1_r)

    linked = (me < n - 1, me > 0)
    aside = (lax.rem(me + 1, n), lax.rem(me + n - 1, n))

    def edge_copy(side, level):
        return pltpu.make_async_remote_copy(
            src_ref=edges.at[side, level], dst_ref=near.at[side, level],
            send_sem=near_s.at[side, level], recv_sem=near_r.at[side, level],
            device_id=(aside[side], core), device_id_type=MESH,
        )

    def tile_copy(side):
        return pltpu.make_async_remote_copy(
            src_ref=info.at[here], dst_ref=beside.at[side],
            send_sem=b_s.at[side], recv_sem=b_r.at[side],
            device_id=(aside[side], core), device_id_type=MESH,
        )

    for side in range(2):

        @pl.when(linked[side])
        def _():
            tile_copy(side).start()

    def edge_sums(level, head, tail):
        def inner_sums(s, nothing):
            at = pl.ds(pl.multiple_of(s * rows, rows), rows)
            block = x[at]
            edges[0, level, at] = jnp.sum(block * tail[None], axis=1)
            edges[1, level, at] = jnp.sum(block * head[None], axis=1)
            return nothing

        lax.fori_loop(0, slices, inner_sums, 0)

    def edge_send(level):
        for side in range(2):

            @pl.when(linked[side])
            def _():
                edge_copy(side, level).start()

    edge_sums(0, head_w, tail_w)
    edge_send(0)
    edge_sums(1, head_m, tail_m)

    def mixed_pair(c, first):
        parts2 = split2(x[pl.ds(c, 2)])
        both = jnp.concatenate([parts2[0], parts2[1]], axis=1)
        return jnp.dot(
            mixer[first * span : (first + 2) * span], both, preferred_element_type=F32
        )

    def mix_far(g, nothing):
        for r in range(0, 8, 2):
            c = g * 8 + r
            mixed = mixed_pair(c, 0)
            for j in range(2):
                own = mixed[:, j * lanes : (j + 1) * lanes]
                run_out[c + j] = own[0:span]
                year_out[c + j] = own[span:]
        return nothing

    lax.fori_loop(0, columns // 8, mix_far, 0)

    from_mates(info, i_s, i_r)
    low = [jnp.broadcast_to(info[b, 7:8, 0:1], (rows, lanes)) for b in range(m)]
    top = [jnp.broadcast_to(info[b, 7:8, 1:2], (rows, lanes)) for b in range(m)]
    from_mates(recv1, s1_s, s1_r)
    zero = jnp.zeros((rows, lanes), F32)

    def cross_copy(peer, both):
        return pltpu.make_async_remote_copy(
            src_ref=half if both else half.at[pl.ds(1, 1)],
            dst_ref=cross.at[here] if both else cross.at[here, pl.ds(1, 1)],
            send_sem=c_s.at[peer], recv_sem=c_r.at[here],
            device_id=(there + peer, core), device_id_type=MESH,
        )

    @pl.when(upper)
    def _():
        leading = zero
        for b in range(m):
            leading = leading + jnp.where(low[b] == low[0], recv1[b, 0], 0.0)
        half[1] = leading
        for j in range(m):
            cross_copy(j, False).start()

    def tail_of(b):
        if wide:
            return recv1[b, 2]
        return jnp.where(low[b] == top[b], recv1[b, 1], recv1[b, 1] - recv1[b, 0])

    running, into = zero, zero
    brought = []
    for b in range(m):
        send2[b, 0] = running
        brought.append(into)
        if wide:
            send2[b, 1] = into
        if b + 1 < m:
            running = running + recv1[b, 1]
            kept = tail_of(b) + jnp.where(low[b] == top[b], into, 0.0)
            into = jnp.where(top[b] == low[b + 1], kept, 0.0)
    back = zero
    for b in reversed(range(m)):
        one = low[b] == top[b]
        if wide:
            send2[b, 2] = back
        else:
            send2[b, 1] = back + jnp.where(one, brought[b], 0.0)
        if b > 0:
            held = recv1[b, 0] + jnp.where(one, back, 0.0)
            back = jnp.where(top[b - 1] == low[b], held, 0.0)
    sent += to_mates(lambda peer: send2.at[peer], carry, s2_s, s2_r)
    carry[here] = send2[here]

    def group_sum(row, chosen):
        value = jnp.zeros((1, lanes), F32)
        for b in range(m):
            value = value + jnp.where(chosen(b), info[b, row : row + 1], 0.0)
        return value

    always = jnp.zeros((1, lanes), F32) == 0.0
    far[0] = stack_rows(
        [
            group_sum(0, lambda b: always),
            group_sum(1, lambda b: low[b][0:1] == low[0][0:1]),
            group_sum(2, lambda b: top[b][0:1] == top[m - 1][0:1]),
            low[0][0:1], top[m - 1][0:1],
        ],
        8, lanes,
    )
    far_copy = pltpu.make_async_remote_copy(
        src_ref=far.at[0], dst_ref=far.at[1], send_sem=f_s, recv_sem=f_r,
        device_id=(there + here, core), device_id_type=MESH,
    )

    @pl.when(lower)
    def _():
        half[0] = running + recv1[m - 1, 1]
        trailing = zero
        for b in range(m):
            trailing = trailing + jnp.where(top[b] == top[m - 1], tail_of(b), 0.0)
        half[1] = trailing
        pl.semaphore_wait(ready, m)
        for j in reversed(range(m)):
            cross_copy(j, True).start()

    far_copy.start()
    edge_send(1)

    for side in range(2):

        @pl.when(linked[1 - side])
        def _():
            tile_copy(side).wait_recv()

    def gain(side, lane_seen, own):
        value = jnp.broadcast_to(beside[side, 7:8, lane_seen : lane_seen + 1], (1, lanes))
        there_is = me > 0 if side == 0 else me < n - 1
        return jnp.where(jnp.logical_and(value == own.astype(F32), there_is), 1.0, 0.0)

    left_w, right_w = head_w * gain(0, 3, week[0]), tail_w * gain(1, 2, week[last])
    left_m, right_m = head_m * gain(0, 5, month[0]), tail_m * gain(1, 4, month[last])
    first_y = head_y if wide else head_y * jnp.where(year[0] == year[last], 0.0, 1.0)
    gains[0] = first_y
    gains[1] = tail_y

    far_copy.wait_recv()
    low_me = jnp.zeros((1, lanes), F32) + year[0].astype(F32)
    top_me = jnp.zeros((1, lanes), F32) + year[last].astype(F32)
    far_low, far_top = far[1, 3:4], far[1, 4:5]
    before = jnp.where(jnp.logical_and(far_top == low_me, upper), 1.0, 0.0)
    after = jnp.where(jnp.logical_and(far_low == top_me, lower), 1.0, 0.0)
    if not wide:
        after = after + before * jnp.where(low_me == top_me, 1.0, 0.0)
    coef[...] = stack_rows([before, after], 8, lanes)
    run_sum = group_sum(0, lambda b: b < here) + jnp.where(upper, far[1, 0:1], 0.0)
    in_sum = group_sum(
        2, lambda b: jnp.logical_and(top[b][0:1] == low_me, b < here)
    ) + before * far[1, 2:3]
    back_sum = group_sum(1, lambda b: jnp.logical_and(low[b][0:1] == top_me, b > here))
    back_sum = back_sum + jnp.where(
        jnp.logical_and(far_low == top_me, lower), far[1, 1:2], 0.0
    )
    if wide:
        first_sum, last_sum = in_sum, back_sum
    else:
        first_sum = run_sum
        last_sum = back_sum + jnp.where(low_me == top_me, in_sum, 0.0)
    parts[core, 0:8] = stack_rows(
        [
            run_sum, first_sum, last_sum,
            beside[0, 4:5], beside[0, 6:7], beside[1, 3:4], beside[1, 5:6],
        ],
        8, lanes,
    )
    parts[core, 8 : 8 + span] = total
    for d in range(1, n_prod):
        peer = lax.rem(core + d, n_prod)
        copy = pltpu.make_async_remote_copy(
            src_ref=parts.at[core], dst_ref=parts.at[core],
            send_sem=sib_s.at[peer], recv_sem=sib_r.at[core],
            device_id=(me, peer), device_id_type=MESH,
        )
        copy.start()
        sent.append(copy)

    for side in range(2):

        @pl.when(linked[1 - side])
        def _():
            for level in range(2):
                edge_copy(side, level).wait_recv()

    def mix_near(g, nothing):
        base_c = pl.multiple_of(g * 8, 8)
        at = pl.ds(base_c, 8)
        from_left_w, from_left_m = near[0, 0, at], near[0, 1, at]
        from_right_w, from_right_m = near[1, 0, at], near[1, 1, at]
        for r in range(0, 8, 2):
            mixed = mixed_pair(base_c + r, 2)
            for j in range(2):
                q = r + j
                row = slice(q, q + 1)
                own = mixed[:, j * lanes : (j + 1) * lanes]
                week_out[base_c + q] = (
                    own[0:span] + from_left_w[row] * left_w + from_right_w[row] * right_w
                )
                month_out[base_c + q] = (
                    own[span:] + from_left_m[row] * left_m + from_right_m[row] * right_m
                )
        return nothing

    lax.fori_loop(0, columns // 8, mix_near, 0)

    for d in range(1, n_prod):
        peer = lax.rem(core + d, n_prod)
        pltpu.make_async_remote_copy(
            src_ref=parts.at[core], dst_ref=parts.at[peer],
            send_sem=sib_s.at[peer], recv_sem=sib_r.at[peer],
            device_id=(me, peer), device_id_type=MESH,
        ).wait_recv()
    whole = parts[0]
    for i in range(1, n_prod):
        whole = whole + parts[i]
    mixed = jnp.dot(mixer[...], split2(whole[8 : 8 + span]), preferred_element_type=F32)
    rollup[0] = mixed[0:span] + whole[0:1]
    rollup[3] = mixed[span : 2 * span] + whole[1:2] * first_y + whole[2:3] * tail_y
    rollup[1] = mixed[2 * span : 3 * span] + whole[3:4] * left_w + whole[5:6] * right_w
    rollup[2] = mixed[3 * span : 4 * span] + whole[4:5] * left_m + whole[6:7] * right_m

    for copy in sent:
        copy.wait_send()
    far_copy.wait_send()
    for side in range(2):

        @pl.when(linked[side])
        def _():
            tile_copy(side).wait_send()
            for level in range(2):
                edge_copy(side, level).wait_send()

    def cross_done(both):
        for j in range(m):
            cross_copy(j, both).wait_send()
        for j in range(m):
            pltpu.make_async_remote_copy(
                src_ref=half.at[pl.ds(1, 1)] if both else half,
                dst_ref=cross.at[j, pl.ds(1, 1)] if both else cross.at[j],
                send_sem=c_s.at[j], recv_sem=c_r.at[j],
                device_id=(there + j, core), device_id_type=MESH,
            ).wait_recv()

    from_mates(carry, s2_s, s2_r)

    @pl.when(lower)
    def _():
        cross_done(True)

    @pl.when(upper)
    def _():
        cross_done(False)


def exchange(n, n_prod, m, slices, wide, week, month, year, sales):
    columns, span, lanes = sales.shape
    rows = columns // slices
    loads = 4 if slices % 4 == 0 else 1
    hbm = pl.BlockSpec(memory_space=pltpu.HBM)
    vmem = pl.BlockSpec(memory_space=pltpu.VMEM)
    packet = (m, 3 if wide else 2, rows, lanes)
    dma = pltpu.SemaphoreType.DMA
    cube = pltpu.VMEM(sales.shape, F32)
    return pl.pallas_call(
        functools.partial(exchange_kernel, n, n_prod, m, slices, loads, wide),
        out_shape=(
            cube, cube, cube, cube,
            pltpu.VMEM(packet, F32),
            pltpu.VMEM((m, 2, rows, lanes), F32),
            pltpu.VMEM((2, span, lanes), F32),
            pltpu.VMEM((8, lanes), F32),
            pltpu.VMEM((4, span, lanes), F32),
        ),
        in_specs=[hbm] * 4,
        out_specs=(vmem,) * 9,
        scratch_shapes=[
            pltpu.SMEM((span,), jnp.int32),
            pltpu.SMEM((span,), jnp.int32),
            pltpu.SMEM((span,), jnp.int32),
            pltpu.VMEM((4 * span, 2 * span), jnp.bfloat16),
            pltpu.VMEM(sales.shape, F32),
            pltpu.VMEM((slices,) + packet[1:], F32),
            pltpu.VMEM(packet, F32),
            pltpu.VMEM(packet, F32),
            pltpu.VMEM((2, rows, lanes), F32),
            pltpu.VMEM((2, 2, columns, lanes), F32),
            pltpu.VMEM((2, 2, columns, lanes), F32),
            pltpu.VMEM((2, 8, lanes), F32),
            pltpu.VMEM((m, 8, lanes), F32),
            pltpu.VMEM((2, 8, lanes), F32),
            pltpu.VMEM((n_prod, 8 + span, lanes), F32),
            dma((3,)), dma((loads,)), pltpu.SemaphoreType.REGULAR,
            dma((m,)), dma((m,)), dma((m,)), dma((m,)), dma((m,)), dma((m,)), dma((m,)), dma((m,)),
            dma, dma, dma((n_prod,)), dma((n_prod,)), dma((2, 2)), dma((2, 2)), dma((2,)), dma((2,)),
        ],
        compiler_params=pltpu.CompilerParams(
            collective_id=0, has_side_effects=True, vmem_limit_bytes=55 << 20
        ),
        name="exchange",
    )(week, month, year, sales)


def apply_kernel(
    wide, slices, steps,
    run_in, week_in, month_in, year_in, carry, cross, gains, coef, rollup_in,
    run_hbm, week_hbm, month_hbm, year_hbm, rollup_hbm,
    run_out, year_out, out_sem, whole_sem,
):
    columns, span, lanes = run_in.shape
    rows = columns // slices
    per_step = slices // steps
    block = columns // steps
    stores = [
        pltpu.make_async_copy(source, target, whole_sem.at[i])
        for i, (source, target) in enumerate(
            ((week_in, week_hbm), (month_in, month_hbm), (rollup_in, rollup_hbm))
        )
    ]
    for copy in stores:
        copy.start()

    def group(g, nothing):
        start = carry[g, 0] + cross[g, 0]
        if wide:
            first = carry[g, 1] + coef[0:1] * cross[g, 1]
            final = carry[g, 2] + coef[1:2] * cross[g, 1]
        else:
            first = start
            final = carry[g, 1] + coef[1:2] * cross[g, 1]
        for r in range(rows):
            c = g * rows + r
            row = slice(r, r + 1)
            run_out[c] = run_in[c] + start[row]
            year_out[c] = year_in[c] + first[row] * gains[0] + final[row] * gains[1]
        return nothing

    for i in range(steps):
        lax.fori_loop(i * per_step, (i + 1) * per_step, group, 0)
        at = pl.ds(i * block, block)
        for k, (source, target) in enumerate(((run_out, run_hbm), (year_out, year_hbm))):
            copy = pltpu.make_async_copy(source.at[at], target.at[at], out_sem.at[i, k])
            copy.start()
            stores.append(copy)
    for copy in stores:
        copy.wait()


def apply(slices, wide, shape, *passed):
    columns, span, lanes = shape
    steps = 8 if slices % 8 == 0 else 1
    hbm = pl.BlockSpec(memory_space=pltpu.HBM)
    vmem = pl.BlockSpec(memory_space=pltpu.VMEM)
    cube_shape = jax.ShapeDtypeStruct(shape, F32)
    cube = pltpu.VMEM(shape, F32)
    dma = pltpu.SemaphoreType.DMA
    return pl.pallas_call(
        functools.partial(apply_kernel, wide, slices, steps),
        out_shape=(cube_shape,) * 4 + (jax.ShapeDtypeStruct((4, span, lanes), F32),),
        in_specs=[vmem] * 9,
        out_specs=(hbm,) * 5,
        scratch_shapes=[cube, cube, dma((steps, 2)), dma((3,))],
        compiler_params=pltpu.CompilerParams(vmem_limit_bytes=16 << 20),
        name="apply",
    )(*passed)


def solution(mesh):
    n, n_prod = mesh.shape["date"], mesh.shape["prod"]

    def local(sales, week, month, year):
        m = n // 2
        slices = min(m, sales.shape[0] // 8)
        wide = n * sales.shape[1] // 300 + 1 > 2
        passed = exchange(n, n_prod, m, slices, wide, week, month, year, sales)
        return apply(slices, wide, sales.shape, *passed)

    return jax.shard_map(
        local,
        mesh=mesh,
        in_specs=(P("prod", "date", None), P("date"), P("date"), P("date")),
        out_specs=(P("prod", "date", None),) * 4 + (P(None, "date", None),),
        check_vma=False,
    )
```

```python
import functools

import jax
import jax.numpy as jnp
from jax import lax
from jax.experimental import pallas as pl
from jax.experimental.pallas import tpu as pltpu
from jax.sharding import PartitionSpec as P

MESH = pl.DeviceIdType.MESH
F32 = jnp.float32


def id_column(ids, span, lanes):
    where = lax.broadcasted_iota(jnp.int32, (span, lanes), 0)
    column = jnp.zeros((span, lanes), jnp.int32)
    for t in range(span):
        column = jnp.where(where == t, ids[t], column)
    return column


def id_row(ids, span, lanes):
    where = lax.broadcasted_iota(jnp.int32, (span, lanes), 1) % span
    row = jnp.zeros((span, lanes), jnp.int32)
    for t in range(span):
        row = jnp.where(where == t, ids[t], row)
    return row


def edge_masks(ids, span, lanes):
    column = id_column(ids, span, lanes)
    return (column == ids[0]).astype(F32), (column == ids[span - 1]).astype(F32)


def stack_rows(values, rows, lanes):
    where = lax.broadcasted_iota(jnp.int32, (rows, lanes), 0)
    tile = jnp.zeros((rows, lanes), F32)
    for i, value in enumerate(values):
        tile = jnp.where(where == i, value, tile)
    return tile


def split2(value):
    high = value.astype(jnp.bfloat16)
    low = (value - high.astype(F32)).astype(jnp.bfloat16)
    return jnp.concatenate([high, low], axis=-2)


def exchange_kernel(
    n, n_prod, m, slices, loads, wide,
    week_hbm, month_hbm, year_hbm, x_hbm,
    run_out, week_out, month_out, year_out, carry, cross, near_m, gains, coef, rollup,
    week, month, year, mixer, x, send1, recv1, send2, half, edges, near_w, beside, info, far, parts,
    ids_sem, load_sem, ready, i_s, i_r, s1_s, s1_r, s2_s, s2_r, c_s, c_r, f_s, f_r, sib_s, sib_r, near_s, near_r, b_s, b_r,
):
    me = lax.axis_index("date")
    core = lax.axis_index("prod")
    columns, span, lanes = x.shape
    rows = columns // slices
    chunk = columns // loads
    last = span - 1
    upper = me >= m
    lower = me < m
    base = jnp.where(upper, m, 0)
    there = m - base
    here = me - base
    order = sorted(range(1, m), key=lambda d: -min(d, m - d))
    loaded = [
        pltpu.make_async_copy(
            x_hbm.at[pl.ds(i * chunk, chunk)], x.at[pl.ds(i * chunk, chunk)], load_sem.at[i]
        )
        for i in range(loads)
    ]
    fetched = [
        pltpu.make_async_copy(source, target, ids_sem.at[i])
        for i, (source, target) in enumerate(
            ((year_hbm, year), (week_hbm, week), (month_hbm, month))
        )
    ]
    for copy in fetched + loaded:
        copy.start()

    barrier = pltpu.get_barrier_semaphore()

    def greet(date, prod):
        pl.semaphore_signal(barrier, inc=1, device_id=(date, prod), device_id_type=MESH)

    @pl.when(lower)
    def _():
        for j in reversed(range(m)):
            greet(m + j, core)

    for d in order:
        greet(base + lax.rem(here + d, m), core)
    for d in range(1, n_prod):
        greet(me, lax.rem(core + d, n_prod))

    @pl.when(me == m)
    def _():
        greet(m - 1, core)

    for copy in fetched:
        copy.wait()
    head_y, tail_y = edge_masks(year, span, lanes)
    head_w, tail_w = edge_masks(week, span, lanes)
    head_m, tail_m = edge_masks(month, span, lanes)
    lane = lax.broadcasted_iota(jnp.int32, (1, lanes), 1)
    ids = jnp.zeros((1, lanes), F32)
    for i, v in enumerate((year[0], year[last], week[0], week[last], month[0], month[last])):
        ids = jnp.where(lane == i, v.astype(F32), ids)
    def outer_sums(s, total):
        block = x[pl.ds(pl.multiple_of(s * rows, rows), rows)]
        send1[s, 0] = jnp.sum(block * head_y[None], axis=1)
        send1[s, 1] = jnp.sum(block, axis=1)
        if wide:
            send1[s, 2] = jnp.sum(block * tail_y[None], axis=1)
        return total + jnp.sum(block, axis=0)

    total = jnp.zeros((span, lanes), F32)
    per_load = slices // loads
    for i in range(loads):
        loaded[i].wait()
        total = lax.fori_loop(i * per_load, (i + 1) * per_load, outer_sums, total)
    info[here] = stack_rows(
        [jnp.sum(total, axis=0, keepdims=True)]
        + [
            jnp.sum(total * mask, axis=0, keepdims=True)
            for mask in (head_y, tail_y, head_w, tail_w, head_m, tail_m)
        ]
        + [ids],
        8, lanes,
    )
    recv1[here] = send1[lax.rem(here, slices)]
    pl.semaphore_wait(
        barrier,
        m - 1 + n_prod - 1 + jnp.where(upper, m, 0) + jnp.where(me == m - 1, 1, 0),
    )

    @pl.when(upper)
    def _():
        for j in range(m):
            pl.semaphore_signal(ready, inc=1, device_id=(j, core), device_id_type=MESH)

    def to_mates(source, target, send_sem, recv_sem):
        copies = []
        for d in order:
            peer = lax.rem(here + d, m)
            copy = pltpu.make_async_remote_copy(
                src_ref=source(peer), dst_ref=target.at[here],
                send_sem=send_sem.at[peer], recv_sem=recv_sem.at[here],
                device_id=(base + peer, core), device_id_type=MESH,
            )
            copy.start()
            copies.append(copy)
        return copies

    def from_mates(target, send_sem, recv_sem):
        for d in order:
            peer = lax.rem(here + d, m)
            pltpu.make_async_remote_copy(
                src_ref=target.at[here], dst_ref=target.at[peer],
                send_sem=send_sem.at[peer], recv_sem=recv_sem.at[peer],
                device_id=(base + peer, core), device_id_type=MESH,
            ).wait_recv()

    sent = to_mates(lambda peer: info.at[here], info, i_s, i_r)
    sent += to_mates(lambda peer: send1.at[lax.rem(peer, slices)], recv1, s1_s, s1_r)

    linked = (me < n - 1, me > 0)
    aside = (lax.rem(me + 1, n), lax.rem(me + n - 1, n))

    def edge_copy(side, level):
        return pltpu.make_async_remote_copy(
            src_ref=edges.at[side, level], dst_ref=(near_w, near_m)[level].at[side],
            send_sem=near_s.at[side, level], recv_sem=near_r.at[side, level],
            device_id=(aside[side], core), device_id_type=MESH,
        )

    def tile_copy(side):
        return pltpu.make_async_remote_copy(
            src_ref=info.at[here], dst_ref=beside.at[side],
            send_sem=b_s.at[side], recv_sem=b_r.at[side],
            device_id=(aside[side], core), device_id_type=MESH,
        )

    for side in range(2):

        @pl.when(linked[side])
        def _():
            tile_copy(side).start()

    @pl.when(lower)
    def _():
        for j in range(m):
            cross[j, 0] = jnp.zeros((rows, lanes), F32)

    @pl.when(me == 0)
    def _():
        near_w[0] = jnp.zeros(near_w.shape[1:], F32)
        near_m[0] = jnp.zeros(near_m.shape[1:], F32)
        beside[0] = jnp.zeros(beside.shape[1:], F32)

    @pl.when(me == n - 1)
    def _():
        near_w[1] = jnp.zeros(near_w.shape[1:], F32)
        near_m[1] = jnp.zeros(near_m.shape[1:], F32)
        beside[1] = jnp.zeros(beside.shape[1:], F32)

    def edge_sums(level, head, tail):
        def inner_sums(s, nothing):
            at = pl.ds(pl.multiple_of(s * rows, rows), rows)
            block = x[at]
            edges[0, level, at] = jnp.sum(block * tail[None], axis=1)
            edges[1, level, at] = jnp.sum(block * head[None], axis=1)
            return nothing

        lax.fori_loop(0, slices, inner_sums, 0)

    def edge_send(level):
        for side in range(2):

            @pl.when(linked[side])
            def _():
                edge_copy(side, level).start()

    edge_sums(0, head_w, tail_w)
    edge_send(0)
    edge_sums(1, head_m, tail_m)
    wider = 2 * span
    sub = lax.broadcasted_iota(jnp.int32, (span, wider), 0)
    place = lax.broadcasted_iota(jnp.int32, (span, wider), 1) % span
    mixer[0:span] = jnp.where(place <= sub, 1.0, 0.0).astype(mixer.dtype)
    for k, level in enumerate((year, week, month)):
        same = id_column(level, span, wider) == id_row(level, span, wider)
        mixer[(k + 1) * span : (k + 2) * span] = jnp.where(same, 1.0, 0.0).astype(mixer.dtype)


    def mixed_pair(c, first):
        parts2 = split2(x[pl.ds(c, 2)])
        both = jnp.concatenate([parts2[0], parts2[1]], axis=1)
        return jnp.dot(
            mixer[first * span : (first + 2) * span], both, preferred_element_type=F32
        )

    stride = min(columns, 32)

    def mix_far(g, nothing):
        for r in range(0, stride, 2):
            c = g * stride + r
            mixed = mixed_pair(c, 0)
            for j in range(2):
                own = mixed[:, j * lanes : (j + 1) * lanes]
                run_out[c + j] = own[0:span]
                year_out[c + j] = own[span:]
        return nothing

    lax.fori_loop(0, columns // stride, mix_far, 0)

    from_mates(info, i_s, i_r)
    low = [jnp.broadcast_to(info[b, 7:8, 0:1], (rows, lanes)) for b in range(m)]
    top = [jnp.broadcast_to(info[b, 7:8, 1:2], (rows, lanes)) for b in range(m)]
    from_mates(recv1, s1_s, s1_r)
    zero = jnp.zeros((rows, lanes), F32)

    def cross_copy(peer, both):
        return pltpu.make_async_remote_copy(
            src_ref=half if both else half.at[pl.ds(1, 1)],
            dst_ref=cross.at[here] if both else cross.at[here, pl.ds(1, 1)],
            send_sem=c_s.at[peer], recv_sem=c_r.at[here],
            device_id=(there + peer, core), device_id_type=MESH,
        )

    @pl.when(upper)
    def _():
        leading = zero
        for b in range(m):
            leading = leading + jnp.where(low[b] == low[0], recv1[b, 0], 0.0)
        half[1] = leading
        for j in range(m):
            cross_copy(j, False).start()

    def tail_of(b):
        if wide:
            return recv1[b, 2]
        return jnp.where(low[b] == top[b], recv1[b, 1], recv1[b, 1] - recv1[b, 0])

    running, into = zero, zero
    brought = []
    for b in range(m):
        send2[b, 0] = running
        brought.append(into)
        if wide:
            send2[b, 1] = into
        if b + 1 < m:
            running = running + recv1[b, 1]
            kept = tail_of(b) + jnp.where(low[b] == top[b], into, 0.0)
            into = jnp.where(top[b] == low[b + 1], kept, 0.0)
    back = zero
    for b in reversed(range(m)):
        one = low[b] == top[b]
        if wide:
            send2[b, 2] = back
        else:
            send2[b, 1] = back + jnp.where(one, brought[b], 0.0)
        if b > 0:
            held = recv1[b, 0] + jnp.where(one, back, 0.0)
            back = jnp.where(top[b - 1] == low[b], held, 0.0)
    sent += to_mates(lambda peer: send2.at[peer], carry, s2_s, s2_r)
    carry[here] = send2[here]

    def group_sum(row, chosen):
        value = jnp.zeros((1, lanes), F32)
        for b in range(m):
            value = value + jnp.where(chosen(b), info[b, row : row + 1], 0.0)
        return value

    always = jnp.zeros((1, lanes), F32) == 0.0
    far[0] = stack_rows(
        [
            group_sum(0, lambda b: always),
            group_sum(1, lambda b: low[b][0:1] == low[0][0:1]),
            group_sum(2, lambda b: top[b][0:1] == top[m - 1][0:1]),
            low[0][0:1], top[m - 1][0:1],
        ],
        8, lanes,
    )
    far_copy = pltpu.make_async_remote_copy(
        src_ref=far.at[0], dst_ref=far.at[1], send_sem=f_s, recv_sem=f_r,
        device_id=(there + here, core), device_id_type=MESH,
    )

    @pl.when(lower)
    def _():
        half[0] = running + recv1[m - 1, 1]
        trailing = zero
        for b in range(m):
            trailing = trailing + jnp.where(top[b] == top[m - 1], tail_of(b), 0.0)
        half[1] = trailing
        pl.semaphore_wait(ready, m)
        for j in reversed(range(m)):
            cross_copy(j, True).start()

    far_copy.start()
    edge_send(1)

    for side in range(2):

        @pl.when(linked[1 - side])
        def _():
            tile_copy(side).wait_recv()

    def gain(side, lane_seen, own):
        value = jnp.broadcast_to(beside[side, 7:8, lane_seen : lane_seen + 1], (1, lanes))
        there_is = me > 0 if side == 0 else me < n - 1
        return jnp.where(jnp.logical_and(value == own.astype(F32), there_is), 1.0, 0.0)

    left_w, right_w = head_w * gain(0, 3, week[0]), tail_w * gain(1, 2, week[last])
    left_m, right_m = head_m * gain(0, 5, month[0]), tail_m * gain(1, 4, month[last])
    first_y = head_y if wide else head_y * jnp.where(year[0] == year[last], 0.0, 1.0)
    gains[0] = first_y
    gains[1] = tail_y
    gains[2] = left_m
    gains[3] = right_m

    for side in range(2):

        @pl.when(linked[1 - side])
        def _():
            edge_copy(side, 0).wait_recv()

    def mix_near(g, nothing):
        for r in range(0, stride, 2):
            mixed = mixed_pair(g * stride + r, 2)
            for j in range(2):
                c = g * stride + r + j
                row = pl.ds(c, 1)
                own = mixed[:, j * lanes : (j + 1) * lanes]
                week_out[c] = own[0:span] + near_w[0, row] * left_w + near_w[1, row] * right_w
                month_out[c] = own[span:]
        return nothing

    lax.fori_loop(0, columns // stride, mix_near, 0)

    far_copy.wait_recv()
    low_me = jnp.zeros((1, lanes), F32) + year[0].astype(F32)
    top_me = jnp.zeros((1, lanes), F32) + year[last].astype(F32)
    far_low, far_top = far[1, 3:4], far[1, 4:5]
    before = jnp.where(jnp.logical_and(far_top == low_me, upper), 1.0, 0.0)
    after = jnp.where(jnp.logical_and(far_low == top_me, lower), 1.0, 0.0)
    if not wide:
        after = after + before * jnp.where(low_me == top_me, 1.0, 0.0)
    coef[...] = stack_rows([before, after], 8, lanes)
    run_sum = group_sum(0, lambda b: b < here) + jnp.where(upper, far[1, 0:1], 0.0)
    in_sum = group_sum(
        2, lambda b: jnp.logical_and(top[b][0:1] == low_me, b < here)
    ) + before * far[1, 2:3]
    back_sum = group_sum(1, lambda b: jnp.logical_and(low[b][0:1] == top_me, b > here))
    back_sum = back_sum + jnp.where(
        jnp.logical_and(far_low == top_me, lower), far[1, 1:2], 0.0
    )
    if wide:
        first_sum, last_sum = in_sum, back_sum
    else:
        first_sum = run_sum
        last_sum = back_sum + jnp.where(low_me == top_me, in_sum, 0.0)
    parts[core, 0:8] = stack_rows(
        [
            run_sum, first_sum, last_sum,
            beside[0, 4:5], beside[0, 6:7], beside[1, 3:4], beside[1, 5:6],
        ],
        8, lanes,
    )
    parts[core, 8 : 8 + span] = total
    for d in range(1, n_prod):
        peer = lax.rem(core + d, n_prod)
        copy = pltpu.make_async_remote_copy(
            src_ref=parts.at[core], dst_ref=parts.at[core],
            send_sem=sib_s.at[peer], recv_sem=sib_r.at[core],
            device_id=(me, peer), device_id_type=MESH,
        )
        copy.start()
        sent.append(copy)

    for d in range(1, n_prod):
        peer = lax.rem(core + d, n_prod)
        pltpu.make_async_remote_copy(
            src_ref=parts.at[core], dst_ref=parts.at[peer],
            send_sem=sib_s.at[peer], recv_sem=sib_r.at[peer],
            device_id=(me, peer), device_id_type=MESH,
        ).wait_recv()
    whole = parts[0]
    for i in range(1, n_prod):
        whole = whole + parts[i]
    mixed = jnp.dot(mixer[...], split2(whole[8 : 8 + span]), preferred_element_type=F32)
    rollup[0] = mixed[0:span] + whole[0:1]
    rollup[3] = mixed[span : 2 * span] + whole[1:2] * first_y + whole[2:3] * tail_y
    rollup[1] = mixed[2 * span : 3 * span] + whole[3:4] * left_w + whole[5:6] * right_w
    rollup[2] = mixed[3 * span : 4 * span] + whole[4:5] * left_m + whole[6:7] * right_m

    for copy in sent:
        copy.wait_send()
    far_copy.wait_send()
    for side in range(2):

        @pl.when(linked[side])
        def _():
            tile_copy(side).wait_send()
            for level in range(2):
                edge_copy(side, level).wait_send()

    def cross_done(both):
        for j in range(m):
            cross_copy(j, both).wait_send()
        for j in range(m):
            pltpu.make_async_remote_copy(
                src_ref=half.at[pl.ds(1, 1)] if both else half,
                dst_ref=cross.at[j, pl.ds(1, 1)] if both else cross.at[j],
                send_sem=c_s.at[j], recv_sem=c_r.at[j],
                device_id=(there + j, core), device_id_type=MESH,
            ).wait_recv()

    for side in range(2):

        @pl.when(linked[1 - side])
        def _():
            edge_copy(side, 1).wait_recv()

    from_mates(carry, s2_s, s2_r)

    @pl.when(lower)
    def _():
        cross_done(True)

    @pl.when(upper)
    def _():
        cross_done(False)


def exchange(n, n_prod, m, slices, wide, week, month, year, sales):
    columns, span, lanes = sales.shape
    rows = columns // slices
    loads = 4 if slices % 4 == 0 else 1
    hbm = pl.BlockSpec(memory_space=pltpu.HBM)
    vmem = pl.BlockSpec(memory_space=pltpu.VMEM)
    packet = (m, 3 if wide else 2, rows, lanes)
    dma = pltpu.SemaphoreType.DMA
    cube = pltpu.VMEM(sales.shape, F32)
    return pl.pallas_call(
        functools.partial(exchange_kernel, n, n_prod, m, slices, loads, wide),
        out_shape=(
            cube, cube, cube, cube,
            pltpu.VMEM(packet, F32),
            pltpu.VMEM((m, 2, rows, lanes), F32),
            pltpu.VMEM((2, columns, lanes), F32),
            pltpu.VMEM((4, span, lanes), F32),
            pltpu.VMEM((8, lanes), F32),
            pltpu.VMEM((4, span, lanes), F32),
        ),
        in_specs=[hbm] * 4,
        out_specs=(vmem,) * 10,
        scratch_shapes=[
            pltpu.SMEM((span,), jnp.int32),
            pltpu.SMEM((span,), jnp.int32),
            pltpu.SMEM((span,), jnp.int32),
            pltpu.VMEM((4 * span, 2 * span), jnp.bfloat16),
            pltpu.VMEM(sales.shape, F32),
            pltpu.VMEM((slices,) + packet[1:], F32),
            pltpu.VMEM(packet, F32),
            pltpu.VMEM(packet, F32),
            pltpu.VMEM((2, rows, lanes), F32),
            pltpu.VMEM((2, 2, columns, lanes), F32),
            pltpu.VMEM((2, columns, lanes), F32),
            pltpu.VMEM((2, 8, lanes), F32),
            pltpu.VMEM((m, 8, lanes), F32),
            pltpu.VMEM((2, 8, lanes), F32),
            pltpu.VMEM((n_prod, 8 + span, lanes), F32),
            dma((3,)), dma((loads,)), pltpu.SemaphoreType.REGULAR,
            dma((m,)), dma((m,)), dma((m,)), dma((m,)), dma((m,)), dma((m,)), dma((m,)), dma((m,)),
            dma, dma, dma((n_prod,)), dma((n_prod,)), dma((2, 2)), dma((2, 2)), dma((2,)), dma((2,)),
        ],
        compiler_params=pltpu.CompilerParams(
            collective_id=0, has_side_effects=True, vmem_limit_bytes=55 << 20
        ),
        name="exchange",
    )(week, month, year, sales)


def apply_kernel(
    wide, slices, steps,
    run_in, week_in, month_in, year_in, carry, cross, near_m, gains, coef, rollup_in,
    run_hbm, week_hbm, month_hbm, year_hbm, rollup_hbm,
    run_out, month_out, year_out, out_sem, whole_sem,
):
    columns, span, lanes = run_in.shape
    rows = columns // slices
    per_step = slices // steps
    block = columns // steps
    stores = [
        pltpu.make_async_copy(source, target, whole_sem.at[i])
        for i, (source, target) in enumerate(
            ((week_in, week_hbm), (rollup_in, rollup_hbm))
        )
    ]
    for copy in stores:
        copy.start()

    def group(g, nothing):
        start = carry[g, 0] + cross[g, 0]
        if wide:
            first = carry[g, 1] + coef[0:1] * cross[g, 1]
            final = carry[g, 2] + coef[1:2] * cross[g, 1]
        else:
            first = start
            final = carry[g, 1] + coef[1:2] * cross[g, 1]
        for r in range(rows):
            c = g * rows + r
            row = slice(r, r + 1)
            side = pl.ds(c, 1)
            run_out[c] = run_in[c] + start[row]
            month_out[c] = month_in[c] + near_m[0, side] * gains[2] + near_m[1, side] * gains[3]
            year_out[c] = year_in[c] + first[row] * gains[0] + final[row] * gains[1]
        return nothing

    for i in range(steps):
        lax.fori_loop(i * per_step, (i + 1) * per_step, group, 0)
        at = pl.ds(i * block, block)
        for k, (source, target) in enumerate(
            ((run_out, run_hbm), (month_out, month_hbm), (year_out, year_hbm))
        ):
            copy = pltpu.make_async_copy(source.at[at], target.at[at], out_sem.at[i, k])
            copy.start()
            stores.append(copy)
    for copy in stores:
        copy.wait()


def apply(slices, wide, shape, *passed):
    columns, span, lanes = shape
    steps = 8 if slices % 8 == 0 else 1
    hbm = pl.BlockSpec(memory_space=pltpu.HBM)
    vmem = pl.BlockSpec(memory_space=pltpu.VMEM)
    cube_shape = jax.ShapeDtypeStruct(shape, F32)
    cube = pltpu.VMEM(shape, F32)
    dma = pltpu.SemaphoreType.DMA
    return pl.pallas_call(
        functools.partial(apply_kernel, wide, slices, steps),
        out_shape=(cube_shape,) * 4 + (jax.ShapeDtypeStruct((4, span, lanes), F32),),
        in_specs=[vmem] * 10,
        out_specs=(hbm,) * 5,
        scratch_shapes=[cube, cube, cube, dma((steps, 3)), dma((2,))],
        compiler_params=pltpu.CompilerParams(vmem_limit_bytes=16 << 20),
        name="apply",
    )(*passed)


def solution(mesh):
    n, n_prod = mesh.shape["date"], mesh.shape["prod"]

    def local(sales, week, month, year):
        m = n // 2
        slices = min(m, sales.shape[0] // 8)
        wide = n * sales.shape[1] // 300 + 1 > 2
        passed = exchange(n, n_prod, m, slices, wide, week, month, year, sales)
        return apply(slices, wide, sales.shape, *passed)

    return jax.shard_map(
        local,
        mesh=mesh,
        in_specs=(P("prod", "date", None), P("date"), P("date"), P("date")),
        out_specs=(P("prod", "date", None),) * 4 + (P(None, "date", None),),
        check_vma=False,
    )
```

```python
import functools

import jax
import jax.numpy as jnp
from jax import lax
from jax.experimental import pallas as pl
from jax.experimental.pallas import tpu as pltpu
from jax.sharding import PartitionSpec as P

MESH = pl.DeviceIdType.MESH
F32 = jnp.float32


def id_column(ids, span, lanes):
    where = lax.broadcasted_iota(jnp.int32, (span, lanes), 0)
    column = jnp.zeros((span, lanes), jnp.int32)
    for t in range(span):
        column = jnp.where(where == t, ids[t], column)
    return column


def id_row(ids, span, lanes):
    where = lax.broadcasted_iota(jnp.int32, (span, lanes), 1) % span
    row = jnp.zeros((span, lanes), jnp.int32)
    for t in range(span):
        row = jnp.where(where == t, ids[t], row)
    return row


def edge_masks(ids, span, lanes):
    column = id_column(ids, span, lanes)
    return (column == ids[0]).astype(F32), (column == ids[span - 1]).astype(F32)


def stack_rows(values, rows, lanes):
    where = lax.broadcasted_iota(jnp.int32, (rows, lanes), 0)
    tile = jnp.zeros((rows, lanes), F32)
    for i, value in enumerate(values):
        tile = jnp.where(where == i, value, tile)
    return tile


def split2(value):
    high = value.astype(jnp.bfloat16)
    low = (value - high.astype(F32)).astype(jnp.bfloat16)
    return jnp.concatenate([high, low], axis=-2)


def exchange_kernel(
    n, n_prod, m, slices, loads, wide,
    week_hbm, month_hbm, year_hbm, x_hbm,
    run_out, week_out, month_out, year_out, carry, cross, near_m, gains, own, far, rollup,
    week, month, year, mixer, x, send1, recv1, send2, half, edges, near_w, beside, info, group, parts,
    ids_sem, load_sem, ready, i_s, i_r, s1_s, s1_r, s2_s, s2_r, c_s, c_r, f_s, f_r, sib_s, sib_r, near_s, near_r, b_s, b_r,
):
    me = lax.axis_index("date")
    core = lax.axis_index("prod")
    columns, span, lanes = x.shape
    rows = columns // slices
    chunk = columns // loads
    last = span - 1
    upper = me >= m
    lower = me < m
    base = jnp.where(upper, m, 0)
    there = m - base
    here = me - base
    nearer = (m + 1) // 2
    farther = jnp.where(here >= nearer, 1, 0)
    order = sorted(range(1, m), key=lambda d: -min(d, m - d))
    loaded = [
        pltpu.make_async_copy(
            x_hbm.at[pl.ds(i * chunk, chunk)], x.at[pl.ds(i * chunk, chunk)], load_sem.at[i]
        )
        for i in range(loads)
    ]
    fetched = [
        pltpu.make_async_copy(source, target, ids_sem.at[i])
        for i, (source, target) in enumerate(
            ((year_hbm, year), (week_hbm, week), (month_hbm, month))
        )
    ]
    for copy in fetched + loaded:
        copy.start()

    barrier = pltpu.get_barrier_semaphore()

    def greet(date, prod):
        pl.semaphore_signal(barrier, inc=1, device_id=(date, prod), device_id_type=MESH)

    @pl.when(lower)
    def _():
        for j in reversed(range(m)):
            greet(m + j, core)
        for d in range(1, n_prod):
            greet(m + here, lax.rem(core + d, n_prod))

    for d in order:
        greet(base + lax.rem(here + d, m), core)
    for d in range(1, n_prod):
        greet(me, lax.rem(core + d, n_prod))

    @pl.when(me == m)
    def _():
        greet(m - 1, core)

    for copy in fetched:
        copy.wait()
    head_y, tail_y = edge_masks(year, span, lanes)
    head_w, tail_w = edge_masks(week, span, lanes)
    head_m, tail_m = edge_masks(month, span, lanes)
    lane = lax.broadcasted_iota(jnp.int32, (1, lanes), 1)
    ids = jnp.zeros((1, lanes), F32)
    for i, v in enumerate((year[0], year[last], week[0], week[last], month[0], month[last])):
        ids = jnp.where(lane == i, v.astype(F32), ids)
    def outer_sums(s, total):
        block = x[pl.ds(pl.multiple_of(s * rows, rows), rows)]
        send1[s, 0] = jnp.sum(block * head_y[None], axis=1)
        send1[s, 1] = jnp.sum(block, axis=1)
        if wide:
            send1[s, 2] = jnp.sum(block * tail_y[None], axis=1)
        return total + jnp.sum(block, axis=0)

    total = jnp.zeros((span, lanes), F32)
    per_load = slices // loads
    for i in range(loads):
        loaded[i].wait()
        total = lax.fori_loop(i * per_load, (i + 1) * per_load, outer_sums, total)
    info[here] = stack_rows(
        [jnp.sum(total, axis=0, keepdims=True)]
        + [
            jnp.sum(total * mask, axis=0, keepdims=True)
            for mask in (head_y, tail_y, head_w, tail_w, head_m, tail_m)
        ]
        + [ids],
        8, lanes,
    )
    recv1[here] = send1[lax.rem(here, slices)]
    pl.semaphore_wait(
        barrier,
        m - 1 + n_prod - 1 + jnp.where(upper, m + n_prod - 1, 0) + jnp.where(me == m - 1, 1, 0),
    )

    @pl.when(upper)
    def _():
        for j in range(m):
            pl.semaphore_signal(
                ready.at[farther], inc=1, device_id=(j, core), device_id_type=MESH
            )
        for d in range(1, n_prod):
            pl.semaphore_signal(
                ready.at[1], inc=1, device_id=(here, lax.rem(core + d, n_prod)),
                device_id_type=MESH,
            )

    def to_mates(source, target, send_sem, recv_sem):
        copies = []
        for d in order:
            peer = lax.rem(here + d, m)
            copy = pltpu.make_async_remote_copy(
                src_ref=source(peer), dst_ref=target.at[here],
                send_sem=send_sem.at[peer], recv_sem=recv_sem.at[here],
                device_id=(base + peer, core), device_id_type=MESH,
            )
            copy.start()
            copies.append(copy)
        return copies

    def from_mates(target, send_sem, recv_sem):
        for d in order:
            peer = lax.rem(here + d, m)
            pltpu.make_async_remote_copy(
                src_ref=target.at[here], dst_ref=target.at[peer],
                send_sem=send_sem.at[peer], recv_sem=recv_sem.at[peer],
                device_id=(base + peer, core), device_id_type=MESH,
            ).wait_recv()

    sent = to_mates(lambda peer: info.at[here], info, i_s, i_r)
    sent += to_mates(lambda peer: send1.at[lax.rem(peer, slices)], recv1, s1_s, s1_r)

    linked = (me < n - 1, me > 0)
    aside = (lax.rem(me + 1, n), lax.rem(me + n - 1, n))

    def edge_copy(side, level):
        return pltpu.make_async_remote_copy(
            src_ref=edges.at[side, level], dst_ref=(near_w, near_m)[level].at[side],
            send_sem=near_s.at[side, level], recv_sem=near_r.at[side, level],
            device_id=(aside[side], core), device_id_type=MESH,
        )

    def tile_copy(side):
        return pltpu.make_async_remote_copy(
            src_ref=info.at[here], dst_ref=beside.at[side],
            send_sem=b_s.at[side], recv_sem=b_r.at[side],
            device_id=(aside[side], core), device_id_type=MESH,
        )

    for side in range(2):

        @pl.when(linked[side])
        def _():
            tile_copy(side).start()

    @pl.when(lower)
    def _():
        for j in range(m):
            cross[j, 0] = jnp.zeros((rows, lanes), F32)

    @pl.when(me == 0)
    def _():
        near_w[0] = jnp.zeros(near_w.shape[1:], F32)
        near_m[0] = jnp.zeros(near_m.shape[1:], F32)
        beside[0] = jnp.zeros(beside.shape[1:], F32)

    @pl.when(me == n - 1)
    def _():
        near_w[1] = jnp.zeros(near_w.shape[1:], F32)
        near_m[1] = jnp.zeros(near_m.shape[1:], F32)
        beside[1] = jnp.zeros(beside.shape[1:], F32)

    def edge_sums(level, head, tail):
        def inner_sums(s, nothing):
            at = pl.ds(pl.multiple_of(s * rows, rows), rows)
            block = x[at]
            edges[0, level, at] = jnp.sum(block * tail[None], axis=1)
            edges[1, level, at] = jnp.sum(block * head[None], axis=1)
            return nothing

        lax.fori_loop(0, slices, inner_sums, 0)

    def edge_send(level):
        for side in range(2):

            @pl.when(linked[side])
            def _():
                edge_copy(side, level).start()

    def edge_send_where(level, where):
        for side in range(2):

            @pl.when(jnp.logical_and(linked[side], where))
            def _():
                edge_copy(side, level).start()

    edge_sums(0, head_w, tail_w)
    edge_send(0)
    edge_sums(1, head_m, tail_m)
    wider = 2 * span
    sub = lax.broadcasted_iota(jnp.int32, (span, wider), 0)
    place = lax.broadcasted_iota(jnp.int32, (span, wider), 1) % span
    mixer[0:span] = jnp.where(place <= sub, 1.0, 0.0).astype(mixer.dtype)
    for k, level in enumerate((year, week, month)):
        same = id_column(level, span, wider) == id_row(level, span, wider)
        mixer[(k + 1) * span : (k + 2) * span] = jnp.where(same, 1.0, 0.0).astype(mixer.dtype)


    def mixed_pair(c, first):
        parts2 = split2(x[pl.ds(c, 2)])
        both = jnp.concatenate([parts2[0], parts2[1]], axis=1)
        return jnp.dot(
            mixer[first * span : (first + 2) * span], both, preferred_element_type=F32
        )

    stride = min(columns, 32)

    def mix_far(g, nothing):
        for r in range(0, stride, 2):
            c = g * stride + r
            mixed = mixed_pair(c, 0)
            for j in range(2):
                own = mixed[:, j * lanes : (j + 1) * lanes]
                run_out[c + j] = own[0:span]
                year_out[c + j] = own[span:]
        return nothing

    lax.fori_loop(0, columns // stride, mix_far, 0)

    from_mates(info, i_s, i_r)
    low = [jnp.broadcast_to(info[b, 7:8, 0:1], (rows, lanes)) for b in range(m)]
    top = [jnp.broadcast_to(info[b, 7:8, 1:2], (rows, lanes)) for b in range(m)]
    from_mates(recv1, s1_s, s1_r)
    zero = jnp.zeros((rows, lanes), F32)

    def cross_copy(peer, both):
        return pltpu.make_async_remote_copy(
            src_ref=half if both else half.at[pl.ds(1, 1)],
            dst_ref=cross.at[here] if both else cross.at[here, pl.ds(1, 1)],
            send_sem=c_s.at[peer], recv_sem=c_r.at[here],
            device_id=(there + peer, core), device_id_type=MESH,
        )

    @pl.when(upper)
    def _():
        leading = zero
        for b in range(m):
            leading = leading + jnp.where(low[b] == low[0], recv1[b, 0], 0.0)
        half[1] = leading
        for j in range(m):
            cross_copy(j, False).start()

    def tail_of(b):
        if wide:
            return recv1[b, 2]
        return jnp.where(low[b] == top[b], recv1[b, 1], recv1[b, 1] - recv1[b, 0])

    running, into = zero, zero
    brought = []
    for b in range(m):
        send2[b, 0] = running
        brought.append(into)
        if wide:
            send2[b, 1] = into
        if b + 1 < m:
            running = running + recv1[b, 1]
            kept = tail_of(b) + jnp.where(low[b] == top[b], into, 0.0)
            into = jnp.where(top[b] == low[b + 1], kept, 0.0)
    back = zero
    for b in reversed(range(m)):
        one = low[b] == top[b]
        if wide:
            send2[b, 2] = back
        else:
            send2[b, 1] = back + jnp.where(one, brought[b], 0.0)
        if b > 0:
            held = recv1[b, 0] + jnp.where(one, back, 0.0)
            back = jnp.where(top[b - 1] == low[b], held, 0.0)
    sent += to_mates(lambda peer: send2.at[peer], carry, s2_s, s2_r)
    edge_send_where(1, me == m - 1)
    carry[here] = send2[here]

    def group_sum(row, chosen):
        value = jnp.zeros((1, lanes), F32)
        for b in range(m):
            value = value + jnp.where(chosen(b), info[b, row : row + 1], 0.0)
        return value

    always = jnp.zeros((1, lanes), F32) == 0.0
    group[...] = stack_rows(
        [
            group_sum(0, lambda b: always),
            group_sum(1, lambda b: low[b][0:1] == low[0][0:1]),
            group_sum(2, lambda b: top[b][0:1] == top[m - 1][0:1]),
            low[0][0:1], top[m - 1][0:1],
        ],
        8, lanes,
    )
    def far_copy(prod):
        return pltpu.make_async_remote_copy(
            src_ref=group, dst_ref=far.at[core], send_sem=f_s.at[prod], recv_sem=f_r.at[core],
            device_id=(there + here, prod), device_id_type=MESH,
        )

    def far_send():
        for prod in range(n_prod):
            far_copy(prod).start()

    @pl.when(upper)
    def _():
        far_send()


    @pl.when(lower)
    def _():
        half[0] = running + recv1[m - 1, 1]
        trailing = zero
        for b in range(m):
            trailing = trailing + jnp.where(top[b] == top[m - 1], tail_of(b), 0.0)
        half[1] = trailing
        pl.semaphore_wait(ready.at[0], nearer)
        pl.semaphore_wait(ready.at[1], m - nearer + n_prod - 1)
        for j in reversed(range(m)):
            cross_copy(j, True).start()
        far_send()

    edge_send_where(1, me != m - 1)

    for side in range(2):

        @pl.when(linked[1 - side])
        def _():
            tile_copy(side).wait_recv()

    def gain(side, lane_seen, own):
        value = jnp.broadcast_to(beside[side, 7:8, lane_seen : lane_seen + 1], (1, lanes))
        there_is = me > 0 if side == 0 else me < n - 1
        return jnp.where(jnp.logical_and(value == own.astype(F32), there_is), 1.0, 0.0)

    left_w, right_w = head_w * gain(0, 3, week[0]), tail_w * gain(1, 2, week[last])
    left_m, right_m = head_m * gain(0, 5, month[0]), tail_m * gain(1, 4, month[last])
    first_y = head_y if wide else head_y * jnp.where(year[0] == year[last], 0.0, 1.0)
    gains[0] = first_y
    gains[1] = tail_y
    gains[2] = left_m
    gains[3] = right_m

    for side in range(2):

        @pl.when(linked[1 - side])
        def _():
            edge_copy(side, 0).wait_recv()

    def mix_near(g, nothing):
        for r in range(0, stride, 2):
            mixed = mixed_pair(g * stride + r, 2)
            for j in range(2):
                c = g * stride + r + j
                row = pl.ds(c, 1)
                own = mixed[:, j * lanes : (j + 1) * lanes]
                week_out[c] = own[0:span] + near_w[0, row] * left_w + near_w[1, row] * right_w
                month_out[c] = own[span:]
        return nothing

    lax.fori_loop(0, columns // stride, mix_near, 0)

    low_me = jnp.zeros((1, lanes), F32) + year[0].astype(F32)
    top_me = jnp.zeros((1, lanes), F32) + year[last].astype(F32)
    one_me = jnp.where(low_me == top_me, 1.0, 0.0)
    run_sum = group_sum(0, lambda b: b < here)
    in_sum = group_sum(2, lambda b: jnp.logical_and(top[b][0:1] == low_me, b < here))
    back_sum = group_sum(1, lambda b: jnp.logical_and(low[b][0:1] == top_me, b > here))
    if not wide:
        back_sum = back_sum + one_me * in_sum
    parts[core, 0:8] = stack_rows(
        [
            run_sum, in_sum, back_sum,
            beside[0, 4:5], beside[0, 6:7], beside[1, 3:4], beside[1, 5:6],
        ],
        8, lanes,
    )
    parts[core, 8 : 8 + span] = total
    for d in range(1, n_prod):
        peer = lax.rem(core + d, n_prod)
        copy = pltpu.make_async_remote_copy(
            src_ref=parts.at[core], dst_ref=parts.at[core],
            send_sem=sib_s.at[peer], recv_sem=sib_r.at[core],
            device_id=(me, peer), device_id_type=MESH,
        )
        copy.start()
        sent.append(copy)

    for d in range(1, n_prod):
        peer = lax.rem(core + d, n_prod)
        pltpu.make_async_remote_copy(
            src_ref=parts.at[core], dst_ref=parts.at[peer],
            send_sem=sib_s.at[peer], recv_sem=sib_r.at[peer],
            device_id=(me, peer), device_id_type=MESH,
        ).wait_recv()
    whole = parts[0]
    for i in range(1, n_prod):
        whole = whole + parts[i]
    mixed = jnp.dot(mixer[...], split2(whole[8 : 8 + span]), preferred_element_type=F32)
    rollup[0] = mixed[0:span]
    rollup[3] = mixed[span : 2 * span]
    rollup[1] = mixed[2 * span : 3 * span] + whole[3:4] * left_w + whole[5:6] * right_w
    rollup[2] = mixed[3 * span : 4 * span] + whole[4:5] * left_m + whole[6:7] * right_m
    own[...] = stack_rows(
        [
            whole[0:1], whole[1:2], whole[2:3], low_me, top_me, one_me,
            jnp.zeros((1, lanes), F32) + jnp.where(upper, 1.0, 0.0),
        ],
        8, lanes,
    )

    for copy in sent:
        copy.wait_send()
    for prod in range(n_prod):
        far_copy(prod).wait_send()
    for side in range(2):

        @pl.when(linked[side])
        def _():
            tile_copy(side).wait_send()
            for level in range(2):
                edge_copy(side, level).wait_send()

    def cross_done(both):
        for j in range(m):
            cross_copy(j, both).wait_send()
        for j in range(m):
            pltpu.make_async_remote_copy(
                src_ref=half.at[pl.ds(1, 1)] if both else half,
                dst_ref=cross.at[j, pl.ds(1, 1)] if both else cross.at[j],
                send_sem=c_s.at[j], recv_sem=c_r.at[j],
                device_id=(there + j, core), device_id_type=MESH,
            ).wait_recv()

    for side in range(2):

        @pl.when(linked[1 - side])
        def _():
            edge_copy(side, 1).wait_recv()

    for prod in range(n_prod):
        pltpu.make_async_remote_copy(
            src_ref=group, dst_ref=far.at[prod], send_sem=f_s.at[prod], recv_sem=f_r.at[prod],
            device_id=(there + here, prod), device_id_type=MESH,
        ).wait_recv()
    from_mates(carry, s2_s, s2_r)

    @pl.when(lower)
    def _():
        cross_done(True)

    @pl.when(upper)
    def _():
        cross_done(False)


def exchange(n, n_prod, m, slices, wide, week, month, year, sales):
    columns, span, lanes = sales.shape
    rows = columns // slices
    loads = 4 if slices % 4 == 0 else 1
    hbm = pl.BlockSpec(memory_space=pltpu.HBM)
    vmem = pl.BlockSpec(memory_space=pltpu.VMEM)
    packet = (m, 3 if wide else 2, rows, lanes)
    dma = pltpu.SemaphoreType.DMA
    cube = pltpu.VMEM(sales.shape, F32)
    return pl.pallas_call(
        functools.partial(exchange_kernel, n, n_prod, m, slices, loads, wide),
        out_shape=(
            cube, cube, cube, cube,
            pltpu.VMEM(packet, F32),
            pltpu.VMEM((m, 2, rows, lanes), F32),
            pltpu.VMEM((2, columns, lanes), F32),
            pltpu.VMEM((4, span, lanes), F32),
            pltpu.VMEM((8, lanes), F32),
            pltpu.VMEM((n_prod, 8, lanes), F32),
            pltpu.VMEM((4, span, lanes), F32),
        ),
        in_specs=[hbm] * 4,
        out_specs=(vmem,) * 11,
        scratch_shapes=[
            pltpu.SMEM((span,), jnp.int32),
            pltpu.SMEM((span,), jnp.int32),
            pltpu.SMEM((span,), jnp.int32),
            pltpu.VMEM((4 * span, 2 * span), jnp.bfloat16),
            pltpu.VMEM(sales.shape, F32),
            pltpu.VMEM((slices,) + packet[1:], F32),
            pltpu.VMEM(packet, F32),
            pltpu.VMEM(packet, F32),
            pltpu.VMEM((2, rows, lanes), F32),
            pltpu.VMEM((2, 2, columns, lanes), F32),
            pltpu.VMEM((2, columns, lanes), F32),
            pltpu.VMEM((2, 8, lanes), F32),
            pltpu.VMEM((m, 8, lanes), F32),
            pltpu.VMEM((8, lanes), F32),
            pltpu.VMEM((n_prod, 8 + span, lanes), F32),
            dma((3,)), dma((loads,)), pltpu.SemaphoreType.REGULAR((2,)),
            dma((m,)), dma((m,)), dma((m,)), dma((m,)), dma((m,)), dma((m,)), dma((m,)), dma((m,)),
            dma((n_prod,)), dma((n_prod,)), dma((n_prod,)), dma((n_prod,)), dma((2, 2)), dma((2, 2)), dma((2,)), dma((2,)),
        ],
        compiler_params=pltpu.CompilerParams(
            collective_id=0, has_side_effects=True, vmem_limit_bytes=55 << 20
        ),
        name="exchange",
    )(week, month, year, sales)


def apply_kernel(
    wide, slices, steps,
    run_in, week_in, month_in, year_in, carry, cross, near_m, gains, own, far, rollup_in,
    run_hbm, week_hbm, month_hbm, year_hbm, rollup_hbm,
    run_out, month_out, year_out, rollup, out_sem, whole_sem,
):
    columns, span, lanes = run_in.shape
    rows = columns // slices
    per_step = slices // steps
    block = columns // steps
    stores = [pltpu.make_async_copy(week_in, week_hbm, whole_sem.at[0])]
    stores[0].start()
    low_me, top_me, one_me, above = own[3:4], own[4:5], own[5:6], own[6:7]
    before = jnp.where(far[0, 4:5] == low_me, above, 0.0)
    after = jnp.where(far[0, 3:4] == top_me, 1.0 - above, 0.0)
    beyond = far[0]
    for prod in range(1, far.shape[0]):
        beyond = beyond + far[prod]
    run_sum = own[0:1] + above * beyond[0:1]
    in_sum = before * beyond[2:3]
    back_sum = own[2:3] + after * beyond[1:2]
    if wide:
        first_sum, last_sum = own[1:2] + in_sum, back_sum
    else:
        first_sum, last_sum = run_sum, back_sum + one_me * in_sum
        after = after + before * one_me
    rollup[0] = rollup_in[0] + run_sum
    rollup[1] = rollup_in[1]
    rollup[2] = rollup_in[2]
    rollup[3] = rollup_in[3] + first_sum * gains[0] + last_sum * gains[1]
    stores.append(pltpu.make_async_copy(rollup, rollup_hbm, whole_sem.at[1]))
    stores[1].start()

    def group(g, nothing):
        start = carry[g, 0] + cross[g, 0]
        if wide:
            first = carry[g, 1] + before * cross[g, 1]
            final = carry[g, 2] + after * cross[g, 1]
        else:
            first = start
            final = carry[g, 1] + after * cross[g, 1]
        for r in range(rows):
            c = g * rows + r
            row = slice(r, r + 1)
            side = pl.ds(c, 1)
            run_out[c] = run_in[c] + start[row]
            month_out[c] = month_in[c] + near_m[0, side] * gains[2] + near_m[1, side] * gains[3]
            year_out[c] = year_in[c] + first[row] * gains[0] + final[row] * gains[1]
        return nothing

    for i in range(steps):
        lax.fori_loop(i * per_step, (i + 1) * per_step, group, 0)
        at = pl.ds(i * block, block)
        for k, (source, target) in enumerate(
            ((run_out, run_hbm), (month_out, month_hbm), (year_out, year_hbm))
        ):
            copy = pltpu.make_async_copy(source.at[at], target.at[at], out_sem.at[i, k])
            copy.start()
            stores.append(copy)
    for copy in stores:
        copy.wait()


def apply(slices, wide, shape, *passed):
    columns, span, lanes = shape
    steps = 4 if slices % 4 == 0 else 1
    hbm = pl.BlockSpec(memory_space=pltpu.HBM)
    vmem = pl.BlockSpec(memory_space=pltpu.VMEM)
    cube_shape = jax.ShapeDtypeStruct(shape, F32)
    cube = pltpu.VMEM(shape, F32)
    dma = pltpu.SemaphoreType.DMA
    return pl.pallas_call(
        functools.partial(apply_kernel, wide, slices, steps),
        out_shape=(cube_shape,) * 4 + (jax.ShapeDtypeStruct((4, span, lanes), F32),),
        in_specs=[vmem] * 11,
        out_specs=(hbm,) * 5,
        scratch_shapes=[
            cube, cube, cube, pltpu.VMEM((4, span, lanes), F32), dma((steps, 3)), dma((2,)),
        ],
        compiler_params=pltpu.CompilerParams(vmem_limit_bytes=16 << 20),
        name="apply",
    )(*passed)


def solution(mesh):
    n, n_prod = mesh.shape["date"], mesh.shape["prod"]

    def local(sales, week, month, year):
        m = n // 2
        slices = min(m, sales.shape[0] // 8)
        wide = n * sales.shape[1] // 300 + 1 > 2
        passed = exchange(n, n_prod, m, slices, wide, week, month, year, sales)
        return apply(slices, wide, sales.shape, *passed)

    return jax.shard_map(
        local,
        mesh=mesh,
        in_specs=(P("prod", "date", None), P("date"), P("date"), P("date")),
        out_specs=(P("prod", "date", None),) * 4 + (P(None, "date", None),),
        check_vma=False,
    )
```

```python
import functools

import jax
import jax.numpy as jnp
from jax import lax
from jax.experimental import pallas as pl
from jax.experimental.pallas import tpu as pltpu
from jax.sharding import PartitionSpec as P

MESH = pl.DeviceIdType.MESH
F32 = jnp.float32


def id_column(ids, span, lanes):
    where = lax.broadcasted_iota(jnp.int32, (span, lanes), 0)
    column = jnp.zeros((span, lanes), jnp.int32)
    for t in range(span):
        column = jnp.where(where == t, ids[t], column)
    return column


def id_row(ids, span, lanes):
    where = lax.broadcasted_iota(jnp.int32, (span, lanes), 1) % span
    row = jnp.zeros((span, lanes), jnp.int32)
    for t in range(span):
        row = jnp.where(where == t, ids[t], row)
    return row


def edge_masks(ids, span, lanes):
    column = id_column(ids, span, lanes)
    return (column == ids[0]).astype(F32), (column == ids[span - 1]).astype(F32)


def stack_rows(values, rows, lanes):
    where = lax.broadcasted_iota(jnp.int32, (rows, lanes), 0)
    tile = jnp.zeros((rows, lanes), F32)
    for i, value in enumerate(values):
        tile = jnp.where(where == i, value, tile)
    return tile


def split2(value):
    high = value.astype(jnp.bfloat16)
    low = (value - high.astype(F32)).astype(jnp.bfloat16)
    return jnp.concatenate([high, low], axis=-2)


def exchange_kernel(
    n, n_prod, m, slices, loads, wide,
    week_hbm, month_hbm, year_hbm, x_hbm,
    run_out, week_out, month_out, year_out, carry, cross, near_m, gains, own, far, rollup,
    week, month, year, mixer, x, send1, recv1, send2, half, edges, near_w, beside, info, group, parts,
    ids_sem, load_sem, ready, i_s, i_r, s1_s, s1_r, s2_s, s2_r, c_s, c_r, f_s, f_r, sib_s, sib_r, near_s, near_r, b_s, b_r,
):
    me = lax.axis_index("date")
    core = lax.axis_index("prod")
    columns, span, lanes = x.shape
    rows = columns // slices
    chunk = columns // loads
    last = span - 1
    upper = me >= m
    lower = me < m
    base = jnp.where(upper, m, 0)
    there = m - base
    here = me - base
    nearer = (m + 1) // 2
    farther = jnp.where(here >= nearer, 1, 0)
    order = sorted(range(1, m), key=lambda d: -min(d, m - d))
    loaded = [
        pltpu.make_async_copy(
            x_hbm.at[pl.ds(i * chunk, chunk)], x.at[pl.ds(i * chunk, chunk)], load_sem.at[i]
        )
        for i in range(loads)
    ]
    fetched = [
        pltpu.make_async_copy(source, target, ids_sem.at[i])
        for i, (source, target) in enumerate(
            ((year_hbm, year), (week_hbm, week), (month_hbm, month))
        )
    ]
    for copy in fetched + loaded:
        copy.start()

    barrier = pltpu.get_barrier_semaphore()

    def greet(date, prod):
        pl.semaphore_signal(barrier, inc=1, device_id=(date, prod), device_id_type=MESH)

    @pl.when(lower)
    def _():
        for j in reversed(range(m)):
            greet(m + j, core)
        for d in range(1, n_prod):
            greet(m + here, lax.rem(core + d, n_prod))

    for d in order:
        greet(base + lax.rem(here + d, m), core)
    for d in range(1, n_prod):
        greet(me, lax.rem(core + d, n_prod))

    @pl.when(me == m)
    def _():
        greet(m - 1, core)

    for copy in fetched:
        copy.wait()
    head_y, tail_y = edge_masks(year, span, lanes)
    head_w, tail_w = edge_masks(week, span, lanes)
    head_m, tail_m = edge_masks(month, span, lanes)
    lane = lax.broadcasted_iota(jnp.int32, (1, lanes), 1)
    ids = jnp.zeros((1, lanes), F32)
    for i, v in enumerate((year[0], year[last], week[0], week[last], month[0], month[last])):
        ids = jnp.where(lane == i, v.astype(F32), ids)
    def outer_sums(s, total):
        block = x[pl.ds(pl.multiple_of(s * rows, rows), rows)]
        send1[s, 0] = jnp.sum(block * head_y[None], axis=1)
        send1[s, 1] = jnp.sum(block, axis=1)
        if wide:
            send1[s, 2] = jnp.sum(block * tail_y[None], axis=1)
        return total + jnp.sum(block, axis=0)

    total = jnp.zeros((span, lanes), F32)
    per_load = slices // loads
    for i in range(loads):
        loaded[i].wait()
        total = lax.fori_loop(i * per_load, (i + 1) * per_load, outer_sums, total)
    info[here] = stack_rows(
        [jnp.sum(total, axis=0, keepdims=True)]
        + [
            jnp.sum(total * mask, axis=0, keepdims=True)
            for mask in (head_y, tail_y, head_w, tail_w, head_m, tail_m)
        ]
        + [ids],
        8, lanes,
    )
    recv1[here] = send1[lax.rem(here, slices)]
    pl.semaphore_wait(
        barrier,
        m - 1 + n_prod - 1 + jnp.where(upper, m + n_prod - 1, 0) + jnp.where(me == m - 1, 1, 0),
    )

    @pl.when(upper)
    def _():
        for j in range(m):
            pl.semaphore_signal(
                ready.at[farther], inc=1, device_id=(j, core), device_id_type=MESH
            )
        for d in range(1, n_prod):
            pl.semaphore_signal(
                ready.at[1], inc=1, device_id=(here, lax.rem(core + d, n_prod)),
                device_id_type=MESH,
            )

    def to_mates(source, target, send_sem, recv_sem):
        copies = []
        for d in order:
            peer = lax.rem(here + d, m)
            copy = pltpu.make_async_remote_copy(
                src_ref=source(peer), dst_ref=target.at[here],
                send_sem=send_sem.at[peer], recv_sem=recv_sem.at[here],
                device_id=(base + peer, core), device_id_type=MESH,
            )
            copy.start()
            copies.append(copy)
        return copies

    def from_mates(target, send_sem, recv_sem):
        for d in order:
            peer = lax.rem(here + d, m)
            pltpu.make_async_remote_copy(
                src_ref=target.at[here], dst_ref=target.at[peer],
                send_sem=send_sem.at[peer], recv_sem=recv_sem.at[peer],
                device_id=(base + peer, core), device_id_type=MESH,
            ).wait_recv()

    sent = to_mates(lambda peer: info.at[here], info, i_s, i_r)
    sent += to_mates(lambda peer: send1.at[lax.rem(peer, slices)], recv1, s1_s, s1_r)

    linked = (me < n - 1, me > 0)
    middle = (me == m - 1, me == m)
    aside = (lax.rem(me + 1, n), lax.rem(me + n - 1, n))

    def edge_copy(side, level):
        return pltpu.make_async_remote_copy(
            src_ref=edges.at[side, level], dst_ref=(near_w, near_m)[level].at[side],
            send_sem=near_s.at[side, level], recv_sem=near_r.at[side, level],
            device_id=(aside[side], core), device_id_type=MESH,
        )

    def tile_copy(side):
        return pltpu.make_async_remote_copy(
            src_ref=info.at[here], dst_ref=beside.at[side],
            send_sem=b_s.at[side], recv_sem=b_r.at[side],
            device_id=(aside[side], core), device_id_type=MESH,
        )

    for side in range(2):

        @pl.when(middle[side])
        def _():
            tile_copy(side).start()

    @pl.when(lower)
    def _():
        for j in range(m):
            cross[j, 0] = jnp.zeros((rows, lanes), F32)

    @pl.when(me == 0)
    def _():
        near_w[0] = jnp.zeros(near_w.shape[1:], F32)
        near_m[0] = jnp.zeros(near_m.shape[1:], F32)
        beside[0] = jnp.zeros(beside.shape[1:], F32)

    @pl.when(me == n - 1)
    def _():
        near_w[1] = jnp.zeros(near_w.shape[1:], F32)
        near_m[1] = jnp.zeros(near_m.shape[1:], F32)
        beside[1] = jnp.zeros(beside.shape[1:], F32)

    def edge_sums(level, head, tail):
        def inner_sums(s, nothing):
            at = pl.ds(pl.multiple_of(s * rows, rows), rows)
            block = x[at]
            edges[0, level, at] = jnp.sum(block * tail[None], axis=1)
            edges[1, level, at] = jnp.sum(block * head[None], axis=1)
            return nothing

        lax.fori_loop(0, slices, inner_sums, 0)

    def edge_send(level):
        for side in range(2):

            @pl.when(linked[side])
            def _():
                edge_copy(side, level).start()

    def edge_send_where(level, where):
        for side in range(2):

            @pl.when(jnp.logical_and(linked[side], where))
            def _():
                edge_copy(side, level).start()

    edge_sums(0, head_w, tail_w)
    edge_send(0)
    edge_sums(1, head_m, tail_m)
    wider = 2 * span
    sub = lax.broadcasted_iota(jnp.int32, (span, wider), 0)
    place = lax.broadcasted_iota(jnp.int32, (span, wider), 1) % span
    mixer[0:span] = jnp.where(place <= sub, 1.0, 0.0).astype(mixer.dtype)
    for k, level in enumerate((year, week, month)):
        same = id_column(level, span, wider) == id_row(level, span, wider)
        mixer[(k + 1) * span : (k + 2) * span] = jnp.where(same, 1.0, 0.0).astype(mixer.dtype)


    def mixed_pair(c, first):
        parts2 = split2(x[pl.ds(c, 2)])
        both = jnp.concatenate([parts2[0], parts2[1]], axis=1)
        return jnp.dot(
            mixer[first * span : (first + 2) * span], both, preferred_element_type=F32
        )

    stride = min(columns, 32)

    def mix_far(g, nothing):
        for r in range(0, stride, 2):
            c = g * stride + r
            mixed = mixed_pair(c, 0)
            for j in range(2):
                own = mixed[:, j * lanes : (j + 1) * lanes]
                run_out[c + j] = own[0:span]
                year_out[c + j] = own[span:]
        return nothing

    lax.fori_loop(0, columns // stride, mix_far, 0)

    from_mates(info, i_s, i_r)
    low = [jnp.broadcast_to(info[b, 7:8, 0:1], (rows, lanes)) for b in range(m)]
    top = [jnp.broadcast_to(info[b, 7:8, 1:2], (rows, lanes)) for b in range(m)]
    from_mates(recv1, s1_s, s1_r)
    zero = jnp.zeros((rows, lanes), F32)

    def cross_copy(peer, both):
        return pltpu.make_async_remote_copy(
            src_ref=half if both else half.at[pl.ds(1, 1)],
            dst_ref=cross.at[here] if both else cross.at[here, pl.ds(1, 1)],
            send_sem=c_s.at[peer], recv_sem=c_r.at[here],
            device_id=(there + peer, core), device_id_type=MESH,
        )

    @pl.when(upper)
    def _():
        leading = zero
        for b in range(m):
            leading = leading + jnp.where(low[b] == low[0], recv1[b, 0], 0.0)
        half[1] = leading
        for j in range(m):
            cross_copy(j, False).start()

    def tail_of(b):
        if wide:
            return recv1[b, 2]
        return jnp.where(low[b] == top[b], recv1[b, 1], recv1[b, 1] - recv1[b, 0])

    running, into = zero, zero
    brought = []
    for b in range(m):
        send2[b, 0] = running
        brought.append(into)
        if wide:
            send2[b, 1] = into
        if b + 1 < m:
            running = running + recv1[b, 1]
            kept = tail_of(b) + jnp.where(low[b] == top[b], into, 0.0)
            into = jnp.where(top[b] == low[b + 1], kept, 0.0)
    back = zero
    for b in reversed(range(m)):
        one = low[b] == top[b]
        if wide:
            send2[b, 2] = back
        else:
            send2[b, 1] = back + jnp.where(one, brought[b], 0.0)
        if b > 0:
            held = recv1[b, 0] + jnp.where(one, back, 0.0)
            back = jnp.where(top[b - 1] == low[b], held, 0.0)
    sent += to_mates(lambda peer: send2.at[peer], carry, s2_s, s2_r)
    edge_send_where(1, me == m - 1)
    carry[here] = send2[here]

    def group_sum(row, chosen):
        value = jnp.zeros((1, lanes), F32)
        for b in range(m):
            value = value + jnp.where(chosen(b), info[b, row : row + 1], 0.0)
        return value

    always = jnp.zeros((1, lanes), F32) == 0.0
    group[...] = stack_rows(
        [
            group_sum(0, lambda b: always),
            group_sum(1, lambda b: low[b][0:1] == low[0][0:1]),
            group_sum(2, lambda b: top[b][0:1] == top[m - 1][0:1]),
            low[0][0:1], top[m - 1][0:1],
        ],
        8, lanes,
    )
    def far_copy(prod):
        return pltpu.make_async_remote_copy(
            src_ref=group, dst_ref=far.at[core], send_sem=f_s.at[prod], recv_sem=f_r.at[core],
            device_id=(there + here, prod), device_id_type=MESH,
        )

    def far_send():
        for prod in range(n_prod):
            far_copy(prod).start()

    @pl.when(upper)
    def _():
        far_send()


    @pl.when(lower)
    def _():
        half[0] = running + recv1[m - 1, 1]
        trailing = zero
        for b in range(m):
            trailing = trailing + jnp.where(top[b] == top[m - 1], tail_of(b), 0.0)
        half[1] = trailing
        pl.semaphore_wait(ready.at[0], nearer)
        pl.semaphore_wait(ready.at[1], m - nearer + n_prod - 1)
        for j in reversed(range(m)):
            cross_copy(j, True).start()
        far_send()

    edge_send_where(1, me != m - 1)

    for side in range(2):

        @pl.when(middle[1 - side])
        def _():
            tile_copy(side).wait_recv()

    @pl.when(here > 0)
    def _():
        beside[0] = info[lax.rem(here + m - 1, m)]

    @pl.when(here < m - 1)
    def _():
        beside[1] = info[lax.rem(here + 1, m)]

    def gain(side, lane_seen, own):
        value = jnp.broadcast_to(beside[side, 7:8, lane_seen : lane_seen + 1], (1, lanes))
        there_is = me > 0 if side == 0 else me < n - 1
        return jnp.where(jnp.logical_and(value == own.astype(F32), there_is), 1.0, 0.0)

    left_w, right_w = head_w * gain(0, 3, week[0]), tail_w * gain(1, 2, week[last])
    left_m, right_m = head_m * gain(0, 5, month[0]), tail_m * gain(1, 4, month[last])
    first_y = head_y if wide else head_y * jnp.where(year[0] == year[last], 0.0, 1.0)
    gains[0] = first_y
    gains[1] = tail_y
    gains[2] = left_m
    gains[3] = right_m

    for side in range(2):

        @pl.when(linked[1 - side])
        def _():
            edge_copy(side, 0).wait_recv()

    def mix_near(g, nothing):
        for r in range(0, stride, 2):
            mixed = mixed_pair(g * stride + r, 2)
            for j in range(2):
                c = g * stride + r + j
                row = pl.ds(c, 1)
                own = mixed[:, j * lanes : (j + 1) * lanes]
                week_out[c] = own[0:span] + near_w[0, row] * left_w + near_w[1, row] * right_w
                month_out[c] = own[span:]
        return nothing

    lax.fori_loop(0, columns // stride, mix_near, 0)

    low_me = jnp.zeros((1, lanes), F32) + year[0].astype(F32)
    top_me = jnp.zeros((1, lanes), F32) + year[last].astype(F32)
    one_me = jnp.where(low_me == top_me, 1.0, 0.0)
    run_sum = group_sum(0, lambda b: b < here)
    in_sum = group_sum(2, lambda b: jnp.logical_and(top[b][0:1] == low_me, b < here))
    back_sum = group_sum(1, lambda b: jnp.logical_and(low[b][0:1] == top_me, b > here))
    if not wide:
        back_sum = back_sum + one_me * in_sum
    parts[core, 0:8] = stack_rows(
        [
            run_sum, in_sum, back_sum,
            beside[0, 4:5], beside[0, 6:7], beside[1, 3:4], beside[1, 5:6],
        ],
        8, lanes,
    )
    parts[core, 8 : 8 + span] = total
    for d in range(1, n_prod):
        peer = lax.rem(core + d, n_prod)
        copy = pltpu.make_async_remote_copy(
            src_ref=parts.at[core], dst_ref=parts.at[core],
            send_sem=sib_s.at[peer], recv_sem=sib_r.at[core],
            device_id=(me, peer), device_id_type=MESH,
        )
        copy.start()
        sent.append(copy)

    for d in range(1, n_prod):
        peer = lax.rem(core + d, n_prod)
        pltpu.make_async_remote_copy(
            src_ref=parts.at[core], dst_ref=parts.at[peer],
            send_sem=sib_s.at[peer], recv_sem=sib_r.at[peer],
            device_id=(me, peer), device_id_type=MESH,
        ).wait_recv()
    whole = parts[0]
    for i in range(1, n_prod):
        whole = whole + parts[i]
    mixed = jnp.dot(mixer[...], split2(whole[8 : 8 + span]), preferred_element_type=F32)
    rollup[0] = mixed[0:span]
    rollup[3] = mixed[span : 2 * span]
    rollup[1] = mixed[2 * span : 3 * span] + whole[3:4] * left_w + whole[5:6] * right_w
    rollup[2] = mixed[3 * span : 4 * span] + whole[4:5] * left_m + whole[6:7] * right_m
    own[...] = stack_rows(
        [
            whole[0:1], whole[1:2], whole[2:3], low_me, top_me, one_me,
            jnp.zeros((1, lanes), F32) + jnp.where(upper, 1.0, 0.0),
        ],
        8, lanes,
    )

    for copy in sent:
        copy.wait_send()
    for prod in range(n_prod):
        far_copy(prod).wait_send()
    for side in range(2):

        @pl.when(linked[side])
        def _():
            @pl.when(middle[side])
            def _():
                tile_copy(side).wait_send()

            for level in range(2):
                edge_copy(side, level).wait_send()

    def cross_done(both):
        for j in range(m):
            cross_copy(j, both).wait_send()
        for j in range(m):
            pltpu.make_async_remote_copy(
                src_ref=half.at[pl.ds(1, 1)] if both else half,
                dst_ref=cross.at[j, pl.ds(1, 1)] if both else cross.at[j],
                send_sem=c_s.at[j], recv_sem=c_r.at[j],
                device_id=(there + j, core), device_id_type=MESH,
            ).wait_recv()

    for side in range(2):

        @pl.when(linked[1 - side])
        def _():
            edge_copy(side, 1).wait_recv()

    for prod in range(n_prod):
        pltpu.make_async_remote_copy(
            src_ref=group, dst_ref=far.at[prod], send_sem=f_s.at[prod], recv_sem=f_r.at[prod],
            device_id=(there + here, prod), device_id_type=MESH,
        ).wait_recv()
    from_mates(carry, s2_s, s2_r)

    @pl.when(lower)
    def _():
        cross_done(True)

    @pl.when(upper)
    def _():
        cross_done(False)


def exchange(n, n_prod, m, slices, wide, week, month, year, sales):
    columns, span, lanes = sales.shape
    rows = columns // slices
    loads = 4 if slices % 4 == 0 else 1
    hbm = pl.BlockSpec(memory_space=pltpu.HBM)
    vmem = pl.BlockSpec(memory_space=pltpu.VMEM)
    packet = (m, 3 if wide else 2, rows, lanes)
    dma = pltpu.SemaphoreType.DMA
    cube = pltpu.VMEM(sales.shape, F32)
    return pl.pallas_call(
        functools.partial(exchange_kernel, n, n_prod, m, slices, loads, wide),
        out_shape=(
            cube, cube, cube, cube,
            pltpu.VMEM(packet, F32),
            pltpu.VMEM((m, 2, rows, lanes), F32),
            pltpu.VMEM((2, columns, lanes), F32),
            pltpu.VMEM((4, span, lanes), F32),
            pltpu.VMEM((8, lanes), F32),
            pltpu.VMEM((n_prod, 8, lanes), F32),
            pltpu.VMEM((4, span, lanes), F32),
        ),
        in_specs=[hbm] * 4,
        out_specs=(vmem,) * 11,
        scratch_shapes=[
            pltpu.SMEM((span,), jnp.int32),
            pltpu.SMEM((span,), jnp.int32),
            pltpu.SMEM((span,), jnp.int32),
            pltpu.VMEM((4 * span, 2 * span), jnp.bfloat16),
            pltpu.VMEM(sales.shape, F32),
            pltpu.VMEM((slices,) + packet[1:], F32),
            pltpu.VMEM(packet, F32),
            pltpu.VMEM(packet, F32),
            pltpu.VMEM((2, rows, lanes), F32),
            pltpu.VMEM((2, 2, columns, lanes), F32),
            pltpu.VMEM((2, columns, lanes), F32),
            pltpu.VMEM((2, 8, lanes), F32),
            pltpu.VMEM((m, 8, lanes), F32),
            pltpu.VMEM((8, lanes), F32),
            pltpu.VMEM((n_prod, 8 + span, lanes), F32),
            dma((3,)), dma((loads,)), pltpu.SemaphoreType.REGULAR((2,)),
            dma((m,)), dma((m,)), dma((m,)), dma((m,)), dma((m,)), dma((m,)), dma((m,)), dma((m,)),
            dma((n_prod,)), dma((n_prod,)), dma((n_prod,)), dma((n_prod,)), dma((2, 2)), dma((2, 2)), dma((2,)), dma((2,)),
        ],
        compiler_params=pltpu.CompilerParams(
            collective_id=0, has_side_effects=True, vmem_limit_bytes=55 << 20
        ),
        name="exchange",
    )(week, month, year, sales)


def apply_kernel(
    wide, slices, steps,
    run_in, week_in, month_in, year_in, carry, cross, near_m, gains, own, far, rollup_in,
    run_hbm, week_hbm, month_hbm, year_hbm, rollup_hbm,
    run_out, month_out, year_out, rollup, out_sem, whole_sem,
):
    columns, span, lanes = run_in.shape
    rows = columns // slices
    per_step = slices // steps
    block = columns // steps
    stores = [pltpu.make_async_copy(week_in, week_hbm, whole_sem.at[0])]
    stores[0].start()
    low_me, top_me, one_me, above = own[3:4], own[4:5], own[5:6], own[6:7]
    before = jnp.where(far[0, 4:5] == low_me, above, 0.0)
    after = jnp.where(far[0, 3:4] == top_me, 1.0 - above, 0.0)
    beyond = far[0]
    for prod in range(1, far.shape[0]):
        beyond = beyond + far[prod]
    run_sum = own[0:1] + above * beyond[0:1]
    in_sum = before * beyond[2:3]
    back_sum = own[2:3] + after * beyond[1:2]
    if wide:
        first_sum, last_sum = own[1:2] + in_sum, back_sum
    else:
        first_sum, last_sum = run_sum, back_sum + one_me * in_sum
        after = after + before * one_me
    rollup[0] = rollup_in[0] + run_sum
    rollup[1] = rollup_in[1]
    rollup[2] = rollup_in[2]
    rollup[3] = rollup_in[3] + first_sum * gains[0] + last_sum * gains[1]
    stores.append(pltpu.make_async_copy(rollup, rollup_hbm, whole_sem.at[1]))
    stores[1].start()

    def group(g, nothing):
        start = carry[g, 0] + cross[g, 0]
        if wide:
            first = carry[g, 1] + before * cross[g, 1]
            final = carry[g, 2] + after * cross[g, 1]
        else:
            first = start
            final = carry[g, 1] + after * cross[g, 1]
        for r in range(rows):
            c = g * rows + r
            row = slice(r, r + 1)
            side = pl.ds(c, 1)
            run_out[c] = run_in[c] + start[row]
            month_out[c] = month_in[c] + near_m[0, side] * gains[2] + near_m[1, side] * gains[3]
            year_out[c] = year_in[c] + first[row] * gains[0] + final[row] * gains[1]
        return nothing

    for i in range(steps):
        lax.fori_loop(i * per_step, (i + 1) * per_step, group, 0)
        at = pl.ds(i * block, block)
        for k, (source, target) in enumerate(
            ((run_out, run_hbm), (month_out, month_hbm), (year_out, year_hbm))
        ):
            copy = pltpu.make_async_copy(source.at[at], target.at[at], out_sem.at[i, k])
            copy.start()
            stores.append(copy)
    for copy in stores:
        copy.wait()


def apply(slices, wide, shape, *passed):
    columns, span, lanes = shape
    steps = 4 if slices % 4 == 0 else 1
    hbm = pl.BlockSpec(memory_space=pltpu.HBM)
    vmem = pl.BlockSpec(memory_space=pltpu.VMEM)
    cube_shape = jax.ShapeDtypeStruct(shape, F32)
    cube = pltpu.VMEM(shape, F32)
    dma = pltpu.SemaphoreType.DMA
    return pl.pallas_call(
        functools.partial(apply_kernel, wide, slices, steps),
        out_shape=(cube_shape,) * 4 + (jax.ShapeDtypeStruct((4, span, lanes), F32),),
        in_specs=[vmem] * 11,
        out_specs=(hbm,) * 5,
        scratch_shapes=[
            cube, cube, cube, pltpu.VMEM((4, span, lanes), F32), dma((steps, 3)), dma((2,)),
        ],
        compiler_params=pltpu.CompilerParams(vmem_limit_bytes=16 << 20),
        name="apply",
    )(*passed)


def solution(mesh):
    n, n_prod = mesh.shape["date"], mesh.shape["prod"]

    def local(sales, week, month, year):
        m = n // 2
        slices = min(m, sales.shape[0] // 8)
        wide = n * sales.shape[1] // 300 + 1 > 2
        passed = exchange(n, n_prod, m, slices, wide, week, month, year, sales)
        return apply(slices, wide, sales.shape, *passed)

    return jax.shard_map(
        local,
        mesh=mesh,
        in_specs=(P("prod", "date", None), P("date"), P("date"), P("date")),
        out_specs=(P("prod", "date", None),) * 4 + (P(None, "date", None),),
        check_vma=False,
    )
```
